512 devices in a mesh: groups: 2 (over y), tm: 32 (over z), height: 8 (over x, core).
Axes of the slice: x: 4, y: 2, z: 32, core: 2. Of those that a mesh axis runs over, the one named last changes fastest.
The devices are a block of a 4x8x32 slice.
Arguments:
- video: bfloat16 [128, 32, 64, 256], P(('groups', 'tm'), 'height'), parts along dimension 0, may hold values from -8 to 8
- norm_gain: float32 [256], replicated, may hold values from 0.25 to 1.75
- spatial_weight: bfloat16 [3, 3, 256, 256], P(None, None, 'height'), may hold values from -0.125 to 0.125
- temporal_weight: bfloat16 [3, 256, 256], replicated, may hold values from -0.21875 to 0.21875
- haar_weight: bfloat16 [2048, 512], replicated, may hold values from -0.125 to 0.125
- query_weight: bfloat16 [512, 512], replicated, may hold values from -1.5 to 1.5
- key_weight: bfloat16 [512, 512], replicated, may hold values from -1.5 to 1.5
Outputs:
- encoded: bfloat16 [64, 16, 32, 512], P(('groups', 'tm'), 'height'), parts along dimension 0
The draws below stay inside these ranges and needn't reach their ends.
There are 2 independent parts, one for each index of `groups`. The reference program is written for one: setup_inputs(seed, part) draws one part's arguments, and reference() takes and returns one part's arrays. A program takes and returns all parts, laid end to end along the dimension named above; an argument that names none is the same for every part. Nothing has to cross between parts.
All inputs are finite; a program needn't handle non-finite values.
Results may differ from the reference program's by a relative error of at most 0.015.
Values may be sent and summed in bfloat16 or wider, within the bound.
No kernel may reach another device: no remote copies, remote signals or barrier semaphores. Data moves between devices by JAX's collectives and lax.ppermute only.
A program may use at most 64 MiB of HBM per device.

```python
import jax
import jax.numpy as jnp
from jax import lax

C = 256
C2 = 512
HEAD_DIM = 64
COLS = 64
FRAMES = 64
ROWS = 32


def draw_video(key, part):
    noise_key = jax.random.fold_in(jax.random.fold_in(key, 11), 0)
    values = jnp.clip(jax.random.normal(noise_key, (FRAMES, ROWS, COLS, C), jnp.float32), -6.0, 6.0)
    return values.astype(jnp.bfloat16)


def attention_pair(key):
    subkeys = jax.random.split(jax.random.fold_in(key, 29), 2)
    spread = C2 ** (-0.5)
    query_own = spread * jax.random.normal(subkeys[0], (C2, C2), jnp.float32)
    key_own = spread * jax.random.normal(subkeys[1], (C2, C2), jnp.float32)
    query_values = jnp.clip(query_own, -6.0 * spread, 6.0 * spread)
    key_values = jnp.clip(key_own, -6.0 * spread, 6.0 * spread)
    return (query_values, key_values)


def draw_query_weight(key, part):
    return attention_pair(key)[0].astype(jnp.bfloat16)


def draw_key_weight(key, part):
    return attention_pair(key)[1].astype(jnp.bfloat16)


def levels(stream_key, shape, cuts, least, high):
    loudness = 1.0
    for dim, blocks in cuts:
        draws = jax.random.uniform(jax.random.fold_in(jax.random.fold_in(stream_key, 6), dim), (blocks,), jnp.float32, least / len(cuts), high / len(cuts))
        loudness = loudness * jnp.repeat(jnp.exp(draws), shape[dim] // blocks).reshape((-1,) + (1,) * (len(shape) - 1 - dim))
    return loudness


def gaussian(rng, dims, scale, limit, cuts=(), held_as=jnp.bfloat16):
    loudness = levels(rng, dims, cuts, -0.22, 0.18) if cuts else 1.0
    values = jax.random.normal(rng, dims, jnp.float32) * scale * loudness
    return jnp.minimum(jnp.maximum(values, -limit), limit).astype(held_as)


def setup_inputs(seed: int = 0, part: int = 0) -> dict:
    key_list = jax.random.split(jax.random.key(seed), 8)
    own_keys = jax.random.split(jax.random.fold_in(key_list[7], part), 8)
    video = draw_video(jax.random.fold_in(jax.random.fold_in(key_list[7], part), 71), part)
    norm_gain = jnp.clip(1.0 + 0.15 * jax.random.normal(key_list[1], (C,), jnp.float32), 0.25, 1.75)
    spatial_weight = gaussian(key_list[2], (3, 3, C, C), (9 * C) ** -0.5, 0.125, ((2, 8),))
    temporal_weight = gaussian(key_list[3], (3, C, C), (3 * C) ** -0.5, 0.21875)
    haar_weight = gaussian(key_list[4], (8 * C, C2), (8 * C) ** -0.5, 0.125)
    query_weight = draw_query_weight(jax.random.fold_in(key_list[7], 71), part)
    key_weight = draw_key_weight(jax.random.fold_in(key_list[7], 71), part)
    return dict(video=video, norm_gain=norm_gain, spatial_weight=spatial_weight, temporal_weight=temporal_weight, haar_weight=haar_weight, query_weight=query_weight, key_weight=key_weight)


epsilon = 1e-06
inv_root = 0.7071067811865476

def activate(video, norm_gain):
    values = video.astype(jnp.float32)
    square = lax.optimization_barrier(jnp.mean(values * values, axis=-1, keepdims=True))
    normed = values * lax.rsqrt(square + epsilon) * norm_gain
    return (normed * jax.nn.sigmoid(normed)).astype(jnp.bfloat16)

def haar_split(values, axis_pos):
    first = lax.index_in_dim(values, 0, axis_pos, keepdims=False)
    second = lax.index_in_dim(values, 1, axis_pos, keepdims=False)
    return jnp.stack([first + second, first - second], axis=axis_pos) * inv_root

def haar_bands(merged):
    frames, rows, columns, channels = merged.shape
    values = merged.astype(jnp.float32).reshape(frames // 2, 2, rows // 2, 2, columns // 2, 2, channels)
    for axis_pos in (1, 3, 5):
        values = haar_split(values, axis_pos)
    values = jnp.transpose(values, (0, 2, 4, 1, 3, 5, 6))
    return values.reshape(frames // 2, rows // 2, columns // 2, 8 * channels).astype(jnp.bfloat16)

def causal_attention(queries, keys, values, head_dim):
    frames, places, width = queries.shape
    heads = width // head_dim
    query_heads = queries.astype(jnp.float32).reshape(frames, places, heads, head_dim)
    key_heads = keys.astype(jnp.float32).reshape(frames, places, heads, head_dim)
    value_heads = values.astype(jnp.float32).reshape(frames, places, heads, head_dim)
    scores = jnp.einsum('tphd,sphd->phts', query_heads, key_heads) * head_dim ** (-0.5)
    order = jnp.arange(frames)
    allowed = order[None, :] <= order[:, None]
    scores = jnp.where(allowed, scores, -1e+30)
    top = lax.optimization_barrier(jnp.max(scores, axis=-1, keepdims=True))
    weights = jnp.exp(scores - top)
    probs = (weights / lax.optimization_barrier(jnp.sum(weights, axis=-1, keepdims=True))).astype(jnp.bfloat16)
    mixed = jnp.einsum('phts,sphd->tphd', probs.astype(jnp.float32), value_heads)
    return mixed.reshape(frames, places, width).astype(jnp.bfloat16)

def reference(video, norm_gain, spatial_weight, temporal_weight, haar_weight, query_weight, key_weight):
    frames, rows, columns, channels = video.shape
    outward = spatial_weight.shape[3]
    acted = activate(video, norm_gain)
    padded = jnp.pad(acted, ((0, 0), (1, 1), (1, 1), (0, 0)))
    total = jnp.zeros((frames * rows * columns, outward), jnp.float32)
    for row_tap in range(3):
        for col_tap in range(3):
            window = padded[:, row_tap:row_tap + rows, col_tap:col_tap + columns, :].reshape(-1, channels)
            total = total + jnp.dot(window, spatial_weight[row_tap, col_tap], preferred_element_type=jnp.float32)
    spatial = total.astype(jnp.bfloat16).reshape(frames, rows, columns, outward)
    extended = jnp.pad(spatial, ((2, 0), (0, 0), (0, 0), (0, 0)))
    temporal = jnp.zeros((frames * rows * columns, channels), jnp.float32)
    for frame_tap in range(3):
        window = extended[frame_tap:frame_tap + frames].reshape(-1, outward)
        temporal = temporal + jnp.dot(window, temporal_weight[frame_tap], preferred_element_type=jnp.float32)
    merged = (video.astype(jnp.float32).reshape(-1, channels) + temporal).astype(jnp.bfloat16)
    bands = haar_bands(merged.reshape(frames, rows, columns, channels))
    coarse_frames, coarse_rows, coarse_cols, band_width = bands.shape
    latent = jnp.dot(bands.reshape(-1, band_width), haar_weight, preferred_element_type=jnp.float32).astype(jnp.bfloat16)
    queries = jnp.dot(latent, query_weight, preferred_element_type=jnp.float32).astype(jnp.bfloat16)
    keys = jnp.dot(latent, key_weight, preferred_element_type=jnp.float32).astype(jnp.bfloat16)
    width = latent.shape[1]
    places = coarse_rows * coarse_cols
    latent_three = latent.reshape(coarse_frames, places, width)
    mixed = causal_attention(queries.reshape(coarse_frames, places, width), keys.reshape(coarse_frames, places, width), latent_three, HEAD_DIM)
    result = (latent_three.astype(jnp.float32) + mixed.astype(jnp.float32)).astype(jnp.bfloat16)
    return result.reshape(coarse_frames, coarse_rows, coarse_cols, width)
```

```python
import jax
import jax.numpy as jnp
from jax import lax
from jax.experimental import pallas as pl
from jax.experimental.pallas import tpu as pltpu
from jax.sharding import PartitionSpec as P

HEAD_DIM = 64
CORES = 2

epsilon = 1e-06
inv_root = 0.7071067811865476

F32 = jnp.float32
BF16 = jnp.bfloat16


def dot(a, b):
    return jnp.dot(a, b, preferred_element_type=F32)


def vmem(count):
    return [pl.BlockSpec(memory_space=pltpu.VMEM) for _ in range(count)]


def params(mib=20):
    return pltpu.CompilerParams(vmem_limit_bytes=mib * 2**20)


def cost(flops, nbytes):
    return pl.CostEstimate(flops=flops, bytes_accessed=nbytes, transcendentals=0)


def prepare_kernel(video_ref, above_ref, below_ref, gain_ref, windows_ref, ordered_ref):
    frames, rows, columns, channels = video_ref.shape
    half = columns // 2
    place = lax.broadcasted_iota(jnp.int32, (3 * columns, columns), 0)
    source = lax.broadcasted_iota(jnp.int32, (3 * columns, columns), 1)
    tap, within = place // columns, place % columns
    wanted = 2 * (within % half) + within // half + tap - 1
    pick = (source == wanted).astype(F32).astype(BF16)
    gain = gain_ref[...]
    for frame in range(frames):
        for row in range(rows + 2):
            if row == 0:
                block = above_ref[frame, 0]
            elif row == rows + 1:
                block = below_ref[frame, 0]
            else:
                block = video_ref[frame, row - 1]
                ordered_ref[frame, row - 1] = dot(pick[columns : 2 * columns], block).astype(BF16)
            values = block.astype(F32)
            square = jnp.mean(values * values, axis=-1, keepdims=True)
            normed = values * lax.rsqrt(square + epsilon) * gain
            acted = (normed * jax.nn.sigmoid(normed)).astype(BF16)
            moved = dot(pick, acted).astype(BF16)
            for t in range(3):
                windows_ref[t, frame, row] = moved[t * columns : (t + 1) * columns]


def haar_rows(values, rows, half):
    out = []
    for pair in range(rows // 2):
        blocks = [
            values[f][((2 * pair + r) * 2 + c) * half : ((2 * pair + r) * 2 + c + 1) * half]
            for f in range(2)
            for r in range(2)
            for c in range(2)
        ]
        for step in (4, 2, 1):
            split = list(blocks)
            for i in range(8):
                if not i & step:
                    split[i] = (blocks[i] + blocks[i + step]) * inv_root
                    split[i + step] = (blocks[i] - blocks[i + step]) * inv_root
            blocks = split
        out.append(jnp.concatenate([b.astype(BF16) for b in blocks], axis=1))
    return jnp.concatenate(out, axis=0)


def spatial_kernel(core_ref, own_ref, other_ref, windows_ref, temporal_ref, haar_ref, spatial_ref, next_ref):
    frames, rows, columns, channels = spatial_ref.shape
    chips = own_ref.shape[0]
    first = core_ref[0] == 0
    taps = []
    for tap in range(9):
        parts = []
        for chip in range(chips):
            own, other = own_ref[chip, tap], other_ref[chip, tap]
            parts += [jnp.where(first, own, other), jnp.where(first, other, own)]
        taps.append(jnp.concatenate(parts, axis=0))
    spatial = []
    for frame in range(frames):
        total = None
        for tap in range(9):
            a, b = tap // 3, tap % 3
            window = windows_ref[b, frame, a : a + rows].reshape(rows * columns, channels)
            term = dot(window, taps[tap])
            total = term if total is None else total + term
        spatial.append(total.astype(BF16))
        spatial_ref[frame] = spatial[-1].reshape(rows, columns, channels)
    early = dot(spatial[0], temporal_ref[0]) + dot(spatial[1], temporal_ref[1])
    late = dot(spatial[1], temporal_ref[0])
    bands = haar_rows([early, late], rows, columns // 2)
    next_ref[...] = dot(bands, haar_ref[...]).astype(BF16)


def latent_kernel(spatial_ref, video_ref, temporal_ref, haar_ref, latent_ref):
    frames, rows, columns, channels = spatial_ref.shape
    first = spatial_ref[0].reshape(rows * columns, channels)
    second = spatial_ref[1].reshape(rows * columns, channels)
    merged = [
        video_ref[0].reshape(rows * columns, channels).astype(F32) + dot(first, temporal_ref[2]),
        video_ref[1].reshape(rows * columns, channels).astype(F32)
        + dot(first, temporal_ref[1])
        + dot(second, temporal_ref[2]),
    ]
    bands = haar_rows(merged, rows, columns // 2)
    latent_ref[...] = dot(bands, haar_ref[...])


def attention_kernel(latent_ref, query_ref, key_ref, out_ref):
    frames = latent_ref.shape[0]
    width = query_ref.shape[0]
    places = latent_ref.shape[1] // width
    rows = places * frames
    latent = jnp.concatenate([latent_ref[:, p * width : (p + 1) * width] for p in range(places)], axis=0)
    queries = dot(latent, query_ref[...]).astype(BF16)
    keys = dot(latent, key_ref[...]).astype(BF16)
    at = lax.broadcasted_iota(jnp.int32, (rows, rows), 0)
    to = lax.broadcasted_iota(jnp.int32, (rows, rows), 1)
    allowed = (at // frames == to // frames) & (to <= at)
    pair = 2 * HEAD_DIM
    lane = lax.broadcasted_iota(jnp.int32, (rows, pair), 1)
    sides = [(lane // HEAD_DIM == i).astype(F32).astype(BF16) for i in range(2)]
    pieces = []
    for start in range(0, width, pair):
        q, k, v = (item[:, start : start + pair] for item in (queries, keys, latent))
        mixed = None
        for side in sides:
            scores = lax.dot_general(q, k * side, (((1,), (1,)), ((), ())), preferred_element_type=F32)
            scores = jnp.where(allowed, scores * HEAD_DIM ** (-0.5), -1e30)
            weights = jnp.exp(scores - jnp.max(scores, axis=-1, keepdims=True))
            probs = (weights / jnp.sum(weights, axis=-1, keepdims=True)).astype(BF16)
            term = dot(probs, v * side)
            mixed = term if mixed is None else mixed + term
        pieces.append((v.astype(F32) + mixed.astype(BF16).astype(F32)).astype(BF16))
    encoded = jnp.concatenate(pieces, axis=1)
    for p in range(places):
        out_ref[:, p * width : (p + 1) * width] = encoded[p * frames : (p + 1) * frames]


def body(video, norm_gain, spatial_weight, temporal_weight, haar_weight, query_weight, key_weight):
    frames, rows, columns, channels = video.shape
    outward = spatial_weight.shape[3]
    width = haar_weight.shape[1]
    height = lax.axis_size("height")
    members = lax.axis_size("tm")
    chips = height // CORES
    slice_depth = spatial_weight.shape[2]

    slices = spatial_weight.reshape(9, slice_depth, outward)
    same_core = [[c + CORES * i for i in range(chips)] for c in range(CORES)]
    own = lax.all_to_all(
        jnp.broadcast_to(slices, (chips, *slices.shape)),
        "height",
        split_axis=0,
        concat_axis=0,
        axis_index_groups=same_core,
        tiled=True,
    )

    above = lax.ppermute(video[:, rows - 1 :], "height", [(i, i + 1) for i in range(height - 1)])
    below = lax.ppermute(video[:, :1], "height", [(i + 1, i) for i in range(height - 1)])
    windows, ordered = pl.pallas_call(
        prepare_kernel,
        out_shape=(
            jax.ShapeDtypeStruct((3, frames, rows + 2, columns, channels), BF16),
            jax.ShapeDtypeStruct(video.shape, BF16),
        ),
        in_specs=vmem(4),
        out_specs=tuple(vmem(2)),
        cost_estimate=cost(2 * 10**9, 4 * 10**6),
        compiler_params=params(),
        name="prepare",
    )(video, above, below, norm_gain.reshape(1, channels))

    own, windows = lax.optimization_barrier((own, windows))
    other = lax.ppermute(own, "height", [(i, i ^ 1) for i in range(height)])
    core = (lax.axis_index("height") % CORES).astype(jnp.int32).reshape(1)
    places = (rows // 2) * (columns // 2)
    spatial, onward = pl.pallas_call(
        spatial_kernel,
        out_shape=(
            jax.ShapeDtypeStruct(video.shape, BF16),
            jax.ShapeDtypeStruct((places, width), BF16),
        ),
        in_specs=[pl.BlockSpec(memory_space=pltpu.SMEM)] + vmem(5),
        out_specs=tuple(vmem(2)),
        cost_estimate=cost(2 * 10**9, 4 * 10**6),
        compiler_params=params(),
        name="spatial",
    )(core, own, other, windows, temporal_weight, haar_weight)

    carried = lax.ppermute(onward, "tm", [(i, i + 1) for i in range(members - 1)])
    latent = pl.pallas_call(
        latent_kernel,
        out_shape=jax.ShapeDtypeStruct((places, width), F32),
        in_specs=vmem(4),
        out_specs=vmem(1)[0],
        cost_estimate=cost(2 * 10**9, 4 * 10**6),
        compiler_params=params(),
        name="latent",
    )(spatial, ordered, temporal_weight, haar_weight)
    latent = (latent + carried.astype(F32)).astype(BF16)

    per_member = places // members
    sent = latent.reshape(per_member, members, width).transpose(1, 0, 2)
    gathered = lax.all_to_all(sent, "tm", split_axis=0, concat_axis=0, tiled=True)
    encoded = pl.pallas_call(
        attention_kernel,
        out_shape=jax.ShapeDtypeStruct((members, per_member * width), BF16),
        in_specs=vmem(3),
        out_specs=vmem(1)[0],
        cost_estimate=cost(10**9, 4 * 10**6),
        compiler_params=params(),
        name="attention",
    )(gathered.reshape(members, per_member * width), query_weight, key_weight)
    returned = lax.all_to_all(
        encoded.reshape(members, per_member, width), "tm", split_axis=0, concat_axis=0, tiled=True
    )
    return returned.transpose(1, 0, 2).reshape(frames // 2, rows // 2, columns // 2, width)


def solution(mesh):
    in_specs = (
        P(("groups", "tm"), "height", None, None),
        P(),
        P(None, None, "height", None),
        P(),
        P(),
        P(),
        P(),
    )
    out_specs = P(("groups", "tm"), "height", None, None)
    return jax.shard_map(body, mesh=mesh, in_specs=in_specs, out_specs=out_specs, check_vma=False)
```

```python
import jax
import jax.numpy as jnp
from jax import lax
from jax.experimental import pallas as pl
from jax.experimental.pallas import tpu as pltpu
from jax.sharding import PartitionSpec as P


HEAD_DIM = 64
CORES = 2

epsilon = 1e-06
inv_root = 0.7071067811865476

F32 = jnp.float32
BF16 = jnp.bfloat16


def dot(a, b):
    return jnp.dot(a, b, preferred_element_type=F32)


def vmem(count):
    return [pl.BlockSpec(memory_space=pltpu.VMEM) for _ in range(count)]


def params(mib=20):
    return pltpu.CompilerParams(vmem_limit_bytes=mib * 2**20)


def cost(flops, nbytes):
    return pl.CostEstimate(flops=flops, bytes_accessed=nbytes, transcendentals=0)


def spread_kernel(slices_ref, video_ref, gain_ref, copies_ref, held_ref, gain_held_ref, sems):
    moves = [(slices_ref, copies_ref.at[i]) for i in range(copies_ref.shape[0])]
    moves += [(video_ref, held_ref), (gain_ref, gain_held_ref)]
    started = [pltpu.make_async_copy(src, dst, sems.at[i]) for i, (src, dst) in enumerate(moves)]
    for copy in started:
        copy.start()
    for copy in started:
        copy.wait()


def edges_kernel(earlier_ref, video_ref, first_ref, last_ref):
    frames, rows = video_ref.shape[:2]
    for i, ref in enumerate((earlier_ref, video_ref)):
        for frame in range(frames):
            first_ref[i * frames + frame] = ref[frame, 0]
            last_ref[i * frames + frame] = ref[frame, rows - 1]


def prepare_kernel(earlier_ref, video_ref, above_ref, below_ref, gain_ref, windows_ref, ordered_ref):
    frames, rows, columns, _ = video_ref.shape
    half = columns // 2
    place = lax.broadcasted_iota(jnp.int32, (3 * columns, columns), 0)
    source = lax.broadcasted_iota(jnp.int32, (3 * columns, columns), 1)
    tap, within = place // columns, place % columns
    wanted = 2 * (within % half) + within // half + tap - 1
    pick = (source == wanted).astype(F32).astype(BF16)
    gain = gain_ref[...]
    for frame in range(2 * frames):
        for row in range(rows + 2):
            if row == 0:
                block = above_ref[frame]
            elif row == rows + 1:
                block = below_ref[frame]
            elif frame < frames:
                block = earlier_ref[frame, row - 1]
            else:
                block = video_ref[frame - frames, row - 1]
                ordered_ref[frame - frames, row - 1] = dot(pick[columns : 2 * columns], block).astype(BF16)
            values = block.astype(F32)
            square = jnp.mean(values * values, axis=-1, keepdims=True)
            normed = values * lax.rsqrt(square + epsilon) * gain
            acted = (normed * jax.nn.sigmoid(normed)).astype(BF16)
            moved = dot(pick, acted).astype(BF16)
            for t in range(3):
                windows_ref[t, frame, row] = moved[t * columns : (t + 1) * columns]


def haar_rows(values, rows, half):
    out = []
    for pair in range(rows // 2):
        blocks = [
            values[f][((2 * pair + r) * 2 + c) * half : ((2 * pair + r) * 2 + c + 1) * half]
            for f in range(2)
            for r in range(2)
            for c in range(2)
        ]
        for step in (4, 2, 1):
            split = list(blocks)
            for i in range(8):
                if not i & step:
                    split[i] = (blocks[i] + blocks[i + step]) * inv_root
                    split[i + step] = (blocks[i] - blocks[i + step]) * inv_root
            blocks = split
        out.append(jnp.concatenate([b.astype(BF16) for b in blocks], axis=1))
    return jnp.concatenate(out, axis=0)


def latent_kernel(core_ref, own_ref, other_ref, windows_ref, video_ref, temporal_ref, haar_ref, latent_ref):
    frames, rows, columns, channels = video_ref.shape
    chips = own_ref.shape[0]
    first = core_ref[0] == 0
    taps = []
    for tap in range(9):
        parts = []
        for chip in range(chips):
            own, other = own_ref[chip, tap], other_ref[chip, tap]
            parts += [jnp.where(first, own, other), jnp.where(first, other, own)]
        taps.append(jnp.concatenate(parts, axis=0))
    spatial = []
    for frame in range(2 * frames):
        total = None
        for tap in range(9):
            a, b = tap // 3, tap % 3
            window = windows_ref[b, frame, a : a + rows].reshape(rows * columns, channels)
            term = dot(window, taps[tap])
            total = term if total is None else total + term
        spatial.append(total.astype(BF16))
    merged = []
    for frame in range(frames):
        total = video_ref[frame].reshape(rows * columns, channels).astype(F32)
        for tap in range(3):
            total = total + dot(spatial[frame + tap], temporal_ref[tap])
        merged.append(total.astype(BF16).astype(F32))
    bands = haar_rows(merged, rows, columns // 2)
    latent_ref[...] = dot(bands, haar_ref[...]).astype(BF16)


def attention_kernel(latent_ref, query_ref, key_ref, out_ref):
    frames = latent_ref.shape[0]
    width = query_ref.shape[0]
    places = latent_ref.shape[1] // width
    rows = places * frames
    latent = jnp.concatenate([latent_ref[:, p * width : (p + 1) * width] for p in range(places)], axis=0)
    queries = dot(latent, query_ref[...]).astype(BF16)
    keys = dot(latent, key_ref[...]).astype(BF16)
    at = lax.broadcasted_iota(jnp.int32, (rows, rows), 0)
    to = lax.broadcasted_iota(jnp.int32, (rows, rows), 1)
    allowed = (at // frames == to // frames) & (to <= at)
    pair = 2 * HEAD_DIM
    lane = lax.broadcasted_iota(jnp.int32, (rows, pair), 1)
    sides = [(lane // HEAD_DIM == i).astype(F32).astype(BF16) for i in range(2)]
    starts = range(0, width, pair)
    scores = []
    for start in starts:
        q, k = queries[:, start : start + pair], keys[:, start : start + pair]
        for side in sides:
            score = lax.dot_general(q, k * side, (((1,), (1,)), ((), ())), preferred_element_type=F32)
            scores.append(jnp.where(allowed, score * HEAD_DIM ** (-0.5), -1e30))
    scores = jnp.concatenate(scores, axis=0)
    weights = jnp.exp(scores - jnp.max(scores, axis=-1, keepdims=True))
    probs = (weights / jnp.sum(weights, axis=-1, keepdims=True)).astype(BF16)
    pieces = []
    for i, start in enumerate(starts):
        v = latent[:, start : start + pair]
        mixed = None
        for j, side in enumerate(sides):
            term = dot(probs[(2 * i + j) * rows : (2 * i + j + 1) * rows], v * side)
            mixed = term if mixed is None else mixed + term
        pieces.append((v.astype(F32) + mixed.astype(BF16).astype(F32)).astype(BF16))
    encoded = jnp.concatenate(pieces, axis=1)
    for p in range(places):
        out_ref[:, p * width : (p + 1) * width] = encoded[p * frames : (p + 1) * frames]


def body(video, norm_gain, spatial_weight, temporal_weight, haar_weight, query_weight, key_weight):
    frames, rows, columns, channels = video.shape
    outward = spatial_weight.shape[3]
    width = haar_weight.shape[1]
    height = lax.axis_size("height")
    members = lax.axis_size("tm")
    chips = height // CORES
    slice_depth = spatial_weight.shape[2]

    earlier = lax.ppermute(video, "tm", [(i, i + 1) for i in range(members - 1)])

    slices = spatial_weight.reshape(9, slice_depth, outward)
    same_core = [[c + CORES * i for i in range(chips)] for c in range(CORES)]
    copies, held, gain = pl.pallas_call(
        spread_kernel,
        out_shape=(
            jax.ShapeDtypeStruct((chips, *slices.shape), BF16),
            jax.ShapeDtypeStruct(video.shape, BF16),
            jax.ShapeDtypeStruct((1, channels), F32),
        ),
        in_specs=[pl.BlockSpec(memory_space=pltpu.HBM)] * 3,
        out_specs=tuple(vmem(3)),
        scratch_shapes=[pltpu.SemaphoreType.DMA((chips + 2,))],
        cost_estimate=cost(10**6, 10**6),
        compiler_params=params(),
        name="spread",
    )(*(pltpu.with_memory_space_constraint(x, pltpu.HBM) for x in (slices, video, norm_gain.reshape(1, channels))))
    own = lax.all_to_all(
        copies, "height", split_axis=0, concat_axis=0, axis_index_groups=same_core, tiled=True
    )

    rims = jax.ShapeDtypeStruct((2 * frames, columns, channels), BF16)
    first, last = pl.pallas_call(
        edges_kernel,
        out_shape=(rims, rims),
        in_specs=vmem(2),
        out_specs=tuple(vmem(2)),
        cost_estimate=cost(10**6, 10**6),
        compiler_params=params(),
        name="edges",
    )(earlier, held)
    above = lax.ppermute(last, "height", [(i, i + 1) for i in range(height - 1)])
    below = lax.ppermute(first, "height", [(i + 1, i) for i in range(height - 1)])
    own, above, below = lax.optimization_barrier((own, above, below))
    windows, ordered = pl.pallas_call(
        prepare_kernel,
        out_shape=(
            jax.ShapeDtypeStruct((3, 2 * frames, rows + 2, columns, channels), BF16),
            jax.ShapeDtypeStruct(video.shape, BF16),
        ),
        in_specs=vmem(5),
        out_specs=tuple(vmem(2)),
        cost_estimate=cost(10**9, 4 * 10**6),
        compiler_params=params(),
        name="prepare",
    )(earlier, held, above, below, gain)

    other = lax.ppermute(own, "height", [(i, i ^ 1) for i in range(height)])
    core = (lax.axis_index("height") % CORES).astype(jnp.int32).reshape(1)
    places = (rows // 2) * (columns // 2)
    latent = pl.pallas_call(
        latent_kernel,
        out_shape=jax.ShapeDtypeStruct((places, width), BF16),
        in_specs=[pl.BlockSpec(memory_space=pltpu.SMEM)] + vmem(6),
        out_specs=vmem(1)[0],
        cost_estimate=cost(4 * 10**9, 8 * 10**6),
        compiler_params=params(),
        name="latent",
    )(core, own, other, windows, ordered, temporal_weight, haar_weight)

    per_member = places // members
    sent = latent.reshape(per_member, members, width).transpose(1, 0, 2)
    gathered = lax.all_to_all(sent, "tm", split_axis=0, concat_axis=0, tiled=True)
    encoded = pl.pallas_call(
        attention_kernel,
        out_shape=jax.ShapeDtypeStruct((members, per_member * width), BF16),
        in_specs=vmem(3),
        out_specs=vmem(1)[0],
        cost_estimate=cost(10**9, 4 * 10**6),
        compiler_params=params(),
        name="attention",
    )(gathered.reshape(members, per_member * width), query_weight, key_weight)
    returned = lax.all_to_all(
        encoded.reshape(members, per_member, width), "tm", split_axis=0, concat_axis=0, tiled=True
    )
    return returned.transpose(1, 0, 2).reshape(frames // 2, rows // 2, columns // 2, width)


def solution(mesh):
    in_specs = (
        P(("groups", "tm"), "height", None, None),
        P(),
        P(None, None, "height", None),
        P(),
        P(),
        P(),
        P(),
    )
    out_specs = P(("groups", "tm"), "height", None, None)

    return jax.shard_map(body, mesh=mesh, in_specs=in_specs, out_specs=out_specs, check_vma=False)
```

```python
import jax
import jax.numpy as jnp
from jax import lax
from jax.experimental import pallas as pl
from jax.experimental.pallas import tpu as pltpu
from jax.sharding import PartitionSpec as P


HEAD_DIM = 64
CORES = 2

epsilon = 1e-06
inv_root = 0.7071067811865476

F32 = jnp.float32
BF16 = jnp.bfloat16


def dot(a, b):
    return jnp.dot(a, b, preferred_element_type=F32)


def vmem(count):
    return [pl.BlockSpec(memory_space=pltpu.VMEM) for _ in range(count)]


def params(mib=20):
    return pltpu.CompilerParams(vmem_limit_bytes=mib * 2**20)


def cost(flops, nbytes):
    return pl.CostEstimate(flops=flops, bytes_accessed=nbytes, transcendentals=0)


def hold_kernel(video_ref, gain_ref, video_held_ref, gain_held_ref, sems):
    moves = [(video_ref, video_held_ref), (gain_ref, gain_held_ref)]
    started = [pltpu.make_async_copy(src, dst, sems.at[i]) for i, (src, dst) in enumerate(moves)]
    for copy in started:
        copy.start()
    for copy in started:
        copy.wait()


def edges_kernel(earlier_ref, video_ref, first_ref, last_ref):
    frames, rows = video_ref.shape[:2]
    for i, ref in enumerate((earlier_ref, video_ref)):
        for frame in range(frames):
            first_ref[i * frames + frame] = ref[frame, 0]
            last_ref[i * frames + frame] = ref[frame, rows - 1]


def far(x):
    return pltpu.with_memory_space_constraint(x, pltpu.HBM)


def prepare_kernel(earlier_ref, video_ref, above_ref, below_ref, gain_ref, windows_ref, ordered_ref):
    frames, rows, columns, _ = video_ref.shape
    half = columns // 2
    place = lax.broadcasted_iota(jnp.int32, (3 * columns, columns), 0)
    source = lax.broadcasted_iota(jnp.int32, (3 * columns, columns), 1)
    tap, within = place // columns, place % columns
    wanted = 2 * (within % half) + within // half + tap - 1
    pick = (source == wanted).astype(F32).astype(BF16)
    gain = gain_ref[...]
    for frame in range(2 * frames):
        for row in range(rows + 2):
            if row == 0:
                block = above_ref[frame]
            elif row == rows + 1:
                block = below_ref[frame]
            elif frame < frames:
                block = earlier_ref[frame, row - 1]
            else:
                block = video_ref[frame - frames, row - 1]
                ordered_ref[frame - frames, row - 1] = dot(pick[columns : 2 * columns], block).astype(BF16)
            values = block.astype(F32)
            square = jnp.mean(values * values, axis=-1, keepdims=True)
            normed = values * lax.rsqrt(square + epsilon) * gain
            acted = (normed * jax.nn.sigmoid(normed)).astype(BF16)
            moved = dot(pick, acted).astype(BF16)
            for t in range(3):
                windows_ref[t, frame, row] = moved[t * columns : (t + 1) * columns]


def haar_rows(values, rows, half):
    out = []
    for pair in range(rows // 2):
        blocks = [
            values[f][((2 * pair + r) * 2 + c) * half : ((2 * pair + r) * 2 + c + 1) * half]
            for f in range(2)
            for r in range(2)
            for c in range(2)
        ]
        for step in (4, 2, 1):
            split = list(blocks)
            for i in range(8):
                if not i & step:
                    split[i] = (blocks[i] + blocks[i + step]) * inv_root
                    split[i + step] = (blocks[i] - blocks[i + step]) * inv_root
            blocks = split
        out.append(jnp.concatenate([b.astype(BF16) for b in blocks], axis=1))
    return jnp.concatenate(out, axis=0)


def latent_kernel(
    core_ref, own_ref, other_ref, windows_ref, video_ref, temporal_far_ref, haar_far_ref, latent_ref, temporal_ref, haar_ref, sems
):
    frames, rows, columns, channels = video_ref.shape
    chips = own_ref.shape[0]
    temporal_copy = pltpu.make_async_copy(temporal_far_ref, temporal_ref, sems.at[0])
    haar_copy = pltpu.make_async_copy(haar_far_ref, haar_ref, sems.at[1])
    temporal_copy.start()
    haar_copy.start()
    first = core_ref[0] == 0
    taps = []
    for tap in range(9):
        parts = []
        for chip in range(chips):
            own, other = own_ref[chip, tap], other_ref[chip, tap]
            parts += [jnp.where(first, own, other), jnp.where(first, other, own)]
        taps.append(jnp.concatenate(parts, axis=0))
    spatial = []
    for frame in range(2 * frames):
        total = None
        for tap in range(9):
            a, b = tap // 3, tap % 3
            window = windows_ref[b, frame, a : a + rows].reshape(rows * columns, channels)
            term = dot(window, taps[tap])
            total = term if total is None else total + term
        spatial.append(total.astype(BF16))
    temporal_copy.wait()
    merged = []
    for frame in range(frames):
        total = video_ref[frame].reshape(rows * columns, channels).astype(F32)
        for tap in range(3):
            total = total + dot(spatial[frame + tap], temporal_ref[tap])
        merged.append(total.astype(BF16).astype(F32))
    bands = haar_rows(merged, rows, columns // 2)
    haar_copy.wait()
    latent_ref[...] = dot(bands, haar_ref[...]).astype(BF16)


def attention_kernel(latent_ref, query_ref, key_ref, out_ref):
    frames = latent_ref.shape[0]
    width = query_ref.shape[0]
    places = latent_ref.shape[1] // width
    rows = places * frames
    latent = jnp.concatenate([latent_ref[:, p * width : (p + 1) * width] for p in range(places)], axis=0)
    queries = dot(latent, query_ref[...]).astype(BF16)
    keys = dot(latent, key_ref[...]).astype(BF16)
    at = lax.broadcasted_iota(jnp.int32, (rows, rows), 0)
    to = lax.broadcasted_iota(jnp.int32, (rows, rows), 1)
    allowed = (at // frames == to // frames) & (to <= at)
    pair = 2 * HEAD_DIM
    lane = lax.broadcasted_iota(jnp.int32, (rows, pair), 1)
    sides = [(lane // HEAD_DIM == i).astype(F32).astype(BF16) for i in range(2)]
    starts = range(0, width, pair)
    scores = []
    for start in starts:
        q, k = queries[:, start : start + pair], keys[:, start : start + pair]
        for side in sides:
            score = lax.dot_general(q, k * side, (((1,), (1,)), ((), ())), preferred_element_type=F32)
            scores.append(jnp.where(allowed, score * HEAD_DIM ** (-0.5), -1e30))
    scores = jnp.concatenate(scores, axis=0)
    weights = jnp.exp(scores - jnp.max(scores, axis=-1, keepdims=True))
    probs = (weights / jnp.sum(weights, axis=-1, keepdims=True)).astype(BF16)
    pieces = []
    for i, start in enumerate(starts):
        v = latent[:, start : start + pair]
        mixed = None
        for j, side in enumerate(sides):
            term = dot(probs[(2 * i + j) * rows : (2 * i + j + 1) * rows], v * side)
            mixed = term if mixed is None else mixed + term
        pieces.append((v.astype(F32) + mixed.astype(BF16).astype(F32)).astype(BF16))
    encoded = jnp.concatenate(pieces, axis=1)
    for p in range(places):
        out_ref[:, p * width : (p + 1) * width] = encoded[p * frames : (p + 1) * frames]


def body(video, norm_gain, spatial_weight, temporal_weight, haar_weight, query_weight, key_weight):
    frames, rows, columns, channels = video.shape
    outward = spatial_weight.shape[3]
    width = haar_weight.shape[1]
    height = lax.axis_size("height")
    members = lax.axis_size("tm")
    chips = height // CORES
    slice_depth = spatial_weight.shape[2]

    earlier = lax.ppermute(video, "tm", [(i, i + 1) for i in range(members - 1)])

    hold = pl.pallas_call(
        hold_kernel,
        out_shape=(
            jax.ShapeDtypeStruct(video.shape, BF16),
            jax.ShapeDtypeStruct((1, channels), F32),
        ),
        in_specs=[pl.BlockSpec(memory_space=pl.ANY)] * 2,
        out_specs=tuple(vmem(2)),
        scratch_shapes=[pltpu.SemaphoreType.DMA((2,))],
        cost_estimate=cost(10**6, 10**6),
        compiler_params=params(),
        name="hold",
    )
    held, gain = hold(far(video), far(norm_gain.reshape(1, channels)))

    slices = spatial_weight.reshape(9, slice_depth, outward)
    same_core = [[c + CORES * i for i in range(chips)] for c in range(CORES)]
    own = lax.all_gather(slices, "height", axis_index_groups=same_core)

    rims = jax.ShapeDtypeStruct((2 * frames, columns, channels), BF16)
    trim = pl.pallas_call(
        edges_kernel,
        out_shape=(rims, rims),
        in_specs=vmem(2),
        out_specs=tuple(vmem(2)),
        cost_estimate=cost(10**6, 10**6),
        compiler_params=params(),
        name="edges",
    )
    first, last = trim(earlier, held)
    above = lax.ppermute(last, "height", [(i, i + 1) for i in range(height - 1)])
    below = lax.ppermute(first, "height", [(i + 1, i) for i in range(height - 1)])
    windows, ordered = pl.pallas_call(
        prepare_kernel,
        out_shape=(
            jax.ShapeDtypeStruct((3, 2 * frames, rows + 2, columns, channels), BF16),
            jax.ShapeDtypeStruct(video.shape, BF16),
        ),
        in_specs=vmem(5),
        out_specs=tuple(vmem(2)),
        cost_estimate=cost(10**9, 4 * 10**6),
        compiler_params=params(),
        name="prepare",
    )(earlier, held, above, below, gain)

    other = lax.ppermute(own, "height", [(i, i ^ 1) for i in range(height)])
    core = (lax.axis_index("height") % CORES).astype(jnp.int32).reshape(1)
    places = (rows // 2) * (columns // 2)
    latent = pl.pallas_call(
        latent_kernel,
        out_shape=jax.ShapeDtypeStruct((places, width), BF16),
        in_specs=[pl.BlockSpec(memory_space=pltpu.SMEM)] + vmem(4) + [pl.BlockSpec(memory_space=pl.ANY)] * 2,
        out_specs=vmem(1)[0],
        scratch_shapes=[
            pltpu.VMEM(temporal_weight.shape, BF16),
            pltpu.VMEM(haar_weight.shape, BF16),
            pltpu.SemaphoreType.DMA((2,)),
        ],
        cost_estimate=cost(4 * 10**9, 8 * 10**6),
        compiler_params=params(),
        name="latent",
    )(core, own, other, windows, ordered, far(temporal_weight), far(haar_weight))

    per_member = places // members
    sent = latent.reshape(per_member, members, width).transpose(1, 0, 2)
    gathered = lax.all_to_all(sent, "tm", split_axis=0, concat_axis=0, tiled=True)
    encoded = pl.pallas_call(
        attention_kernel,
        out_shape=jax.ShapeDtypeStruct((members, per_member * width), BF16),
        in_specs=vmem(3),
        out_specs=vmem(1)[0],
        cost_estimate=cost(10**9, 4 * 10**6),
        compiler_params=params(),
        name="attention",
    )(gathered.reshape(members, per_member * width), query_weight, key_weight)
    returned = lax.all_to_all(
        encoded.reshape(members, per_member, width), "tm", split_axis=0, concat_axis=0, tiled=True
    )
    return returned.transpose(1, 0, 2).reshape(frames // 2, rows // 2, columns // 2, width)


def solution(mesh):
    in_specs = (
        P(("groups", "tm"), "height", None, None),
        P(),
        P(None, None, "height", None),
        P(),
        P(),
        P(),
        P(),
    )
    out_specs = P(("groups", "tm"), "height", None, None)

    return jax.shard_map(body, mesh=mesh, in_specs=in_specs, out_specs=out_specs, check_vma=False)
```

```python
import jax
import jax.numpy as jnp
from jax import lax
from jax.experimental import pallas as pl
from jax.experimental.pallas import tpu as pltpu
from jax.sharding import PartitionSpec as P


HEAD_DIM = 64
CORES = 2

epsilon = 1e-06
inv_root = 0.7071067811865476

F32 = jnp.float32
BF16 = jnp.bfloat16


def dot(a, b):
    return jnp.dot(a, b, preferred_element_type=F32)


def vmem(count):
    return [pl.BlockSpec(memory_space=pltpu.VMEM) for _ in range(count)]


def params(mib=20):
    return pltpu.CompilerParams(vmem_limit_bytes=mib * 2**20)


def cost(flops, nbytes):
    return pl.CostEstimate(flops=flops, bytes_accessed=nbytes, transcendentals=0)


def spread_kernel(slices_ref, video_ref, gain_ref, copies_ref, held_ref, gain_held_ref, sems):
    moves = [(slices_ref, copies_ref.at[i]) for i in range(copies_ref.shape[0])]
    moves += [(video_ref, held_ref), (gain_ref, gain_held_ref)]
    started = [pltpu.make_async_copy(src, dst, sems.at[i]) for i, (src, dst) in enumerate(moves)]
    for copy in started:
        copy.start()
    for copy in started:
        copy.wait()


def edges_kernel(earlier_ref, video_ref, first_ref, last_ref):
    frames, rows = video_ref.shape[:2]
    for i, ref in enumerate((earlier_ref, video_ref)):
        for frame in range(frames):
            first_ref[i * frames + frame] = ref[frame, 0]
            last_ref[i * frames + frame] = ref[frame, rows - 1]


def far(x):
    return pltpu.with_memory_space_constraint(x, pltpu.HBM)


def prepare_kernel(earlier_ref, video_ref, above_ref, below_ref, gain_ref, windows_ref, ordered_ref):
    frames, rows, columns, _ = video_ref.shape
    half = columns // 2
    place = lax.broadcasted_iota(jnp.int32, (3 * columns, columns), 0)
    source = lax.broadcasted_iota(jnp.int32, (3 * columns, columns), 1)
    tap, within = place // columns, place % columns
    wanted = 2 * (within % half) + within // half + tap - 1
    pick = (source == wanted).astype(F32).astype(BF16)
    gain = gain_ref[...]
    for frame in range(2 * frames):
        for row in range(rows + 2):
            if row == 0:
                block = above_ref[frame]
            elif row == rows + 1:
                block = below_ref[frame]
            elif frame < frames:
                block = earlier_ref[frame, row - 1]
            else:
                block = video_ref[frame - frames, row - 1]
                ordered_ref[frame - frames, row - 1] = dot(pick[columns : 2 * columns], block).astype(BF16)
            values = block.astype(F32)
            square = jnp.mean(values * values, axis=-1, keepdims=True)
            normed = values * lax.rsqrt(square + epsilon) * gain
            acted = (normed * jax.nn.sigmoid(normed)).astype(BF16)
            moved = dot(pick, acted).astype(BF16)
            for t in range(3):
                windows_ref[t, frame, row] = moved[t * columns : (t + 1) * columns]


def haar_rows(values, rows, half):
    out = []
    for pair in range(rows // 2):
        blocks = [
            values[f][((2 * pair + r) * 2 + c) * half : ((2 * pair + r) * 2 + c + 1) * half]
            for f in range(2)
            for r in range(2)
            for c in range(2)
        ]
        for step in (4, 2, 1):
            split = list(blocks)
            for i in range(8):
                if not i & step:
                    split[i] = (blocks[i] + blocks[i + step]) * inv_root
                    split[i + step] = (blocks[i] - blocks[i + step]) * inv_root
            blocks = split
        out.append(jnp.concatenate([b.astype(BF16) for b in blocks], axis=1))
    return jnp.concatenate(out, axis=0)


def latent_kernel(
    core_ref, own_ref, other_ref, windows_ref, video_ref, temporal_far_ref, haar_far_ref, latent_ref, temporal_ref, haar_ref, sems
):
    frames, rows, columns, channels = video_ref.shape
    chips = own_ref.shape[0]
    temporal_copy = pltpu.make_async_copy(temporal_far_ref, temporal_ref, sems.at[0])
    haar_copy = pltpu.make_async_copy(haar_far_ref, haar_ref, sems.at[1])
    temporal_copy.start()
    haar_copy.start()
    first = core_ref[0] == 0
    taps = []
    for tap in range(9):
        parts = []
        for chip in range(chips):
            own, other = own_ref[chip, tap], other_ref[chip, tap]
            parts += [jnp.where(first, own, other), jnp.where(first, other, own)]
        taps.append(jnp.concatenate(parts, axis=0))
    spatial = []
    for frame in range(2 * frames):
        total = None
        for tap in range(9):
            a, b = tap // 3, tap % 3
            window = windows_ref[b, frame, a : a + rows].reshape(rows * columns, channels)
            term = dot(window, taps[tap])
            total = term if total is None else total + term
        spatial.append(total.astype(BF16))
    temporal_copy.wait()
    merged = []
    for frame in range(frames):
        total = video_ref[frame].reshape(rows * columns, channels).astype(F32)
        for tap in range(3):
            total = total + dot(spatial[frame + tap], temporal_ref[tap])
        merged.append(total.astype(BF16).astype(F32))
    bands = haar_rows(merged, rows, columns // 2)
    haar_copy.wait()
    latent_ref[...] = dot(bands, haar_ref[...]).astype(BF16)


def attention_kernel(latent_ref, query_ref, key_ref, out_ref):
    frames = latent_ref.shape[0]
    width = query_ref.shape[0]
    places = latent_ref.shape[1] // width
    rows = places * frames
    latent = jnp.concatenate([latent_ref[:, p * width : (p + 1) * width] for p in range(places)], axis=0)
    queries = dot(latent, query_ref[...]).astype(BF16)
    keys = dot(latent, key_ref[...]).astype(BF16)
    at = lax.broadcasted_iota(jnp.int32, (rows, rows), 0)
    to = lax.broadcasted_iota(jnp.int32, (rows, rows), 1)
    allowed = (at // frames == to // frames) & (to <= at)
    pair = 2 * HEAD_DIM
    lane = lax.broadcasted_iota(jnp.int32, (rows, pair), 1)
    sides = [(lane // HEAD_DIM == i).astype(F32).astype(BF16) for i in range(2)]
    starts = range(0, width, pair)
    scores = []
    for start in starts:
        q, k = queries[:, start : start + pair], keys[:, start : start + pair]
        for side in sides:
            score = lax.dot_general(q, k * side, (((1,), (1,)), ((), ())), preferred_element_type=F32)
            scores.append(jnp.where(allowed, score * HEAD_DIM ** (-0.5), -1e30))
    scores = jnp.concatenate(scores, axis=0)
    weights = jnp.exp(scores - jnp.max(scores, axis=-1, keepdims=True))
    probs = (weights / jnp.sum(weights, axis=-1, keepdims=True)).astype(BF16)
    pieces = []
    for i, start in enumerate(starts):
        v = latent[:, start : start + pair]
        mixed = None
        for j, side in enumerate(sides):
            term = dot(probs[(2 * i + j) * rows : (2 * i + j + 1) * rows], v * side)
            mixed = term if mixed is None else mixed + term
        pieces.append((v.astype(F32) + mixed.astype(BF16).astype(F32)).astype(BF16))
    encoded = jnp.concatenate(pieces, axis=1)
    for p in range(places):
        out_ref[:, p * width : (p + 1) * width] = encoded[p * frames : (p + 1) * frames]


def body(video, norm_gain, spatial_weight, temporal_weight, haar_weight, query_weight, key_weight):
    frames, rows, columns, channels = video.shape
    outward = spatial_weight.shape[3]
    width = haar_weight.shape[1]
    height = lax.axis_size("height")
    members = lax.axis_size("tm")
    chips = height // CORES
    slice_depth = spatial_weight.shape[2]

    earlier = lax.ppermute(video, "tm", [(i, i + 1) for i in range(members - 1)])

    slices = spatial_weight.reshape(9, slice_depth, outward)
    same_core = [[c + CORES * i for i in range(chips)] for c in range(CORES)]
    copies, held, gain = pl.pallas_call(
        spread_kernel,
        out_shape=(
            jax.ShapeDtypeStruct((chips, *slices.shape), BF16),
            jax.ShapeDtypeStruct(video.shape, BF16),
            jax.ShapeDtypeStruct((1, channels), F32),
        ),
        in_specs=[pl.BlockSpec(memory_space=pltpu.HBM)] * 3,
        out_specs=tuple(vmem(3)),
        scratch_shapes=[pltpu.SemaphoreType.DMA((chips + 2,))],
        cost_estimate=cost(10**6, 10**6),
        compiler_params=params(),
        name="spread",
    )(far(slices), far(video), far(norm_gain.reshape(1, channels)))
    own = lax.all_to_all(
        copies, "height", split_axis=0, concat_axis=0, axis_index_groups=same_core, tiled=True
    )

    rims = jax.ShapeDtypeStruct((2 * frames, columns, channels), BF16)
    trim = pl.pallas_call(
        edges_kernel,
        out_shape=(rims, rims),
        in_specs=vmem(2),
        out_specs=tuple(vmem(2)),
        cost_estimate=cost(10**6, 10**6),
        compiler_params=params(),
        name="edges",
    )
    first, last = trim(earlier, held)
    above = lax.ppermute(last, "height", [(i, i + 1) for i in range(height - 1)])
    below = lax.ppermute(first, "height", [(i + 1, i) for i in range(height - 1)])
    windows, ordered = pl.pallas_call(
        prepare_kernel,
        out_shape=(
            jax.ShapeDtypeStruct((3, 2 * frames, rows + 2, columns, channels), BF16),
            jax.ShapeDtypeStruct(video.shape, BF16),
        ),
        in_specs=vmem(5),
        out_specs=tuple(vmem(2)),
        cost_estimate=cost(10**9, 4 * 10**6),
        compiler_params=params(),
        name="prepare",
    )(earlier, held, above, below, gain)

    other = lax.ppermute(own, "height", [(i, i ^ 1) for i in range(height)])
    core = (lax.axis_index("height") % CORES).astype(jnp.int32).reshape(1)
    places = (rows // 2) * (columns // 2)
    latent = pl.pallas_call(
        latent_kernel,
        out_shape=jax.ShapeDtypeStruct((places, width), BF16),
        in_specs=[pl.BlockSpec(memory_space=pltpu.SMEM)] + vmem(4) + [pl.BlockSpec(memory_space=pl.ANY)] * 2,
        out_specs=vmem(1)[0],
        scratch_shapes=[
            pltpu.VMEM(temporal_weight.shape, BF16),
            pltpu.VMEM(haar_weight.shape, BF16),
            pltpu.SemaphoreType.DMA((2,)),
        ],
        cost_estimate=cost(4 * 10**9, 8 * 10**6),
        compiler_params=params(),
        name="latent",
    )(core, own, other, windows, ordered, far(temporal_weight), far(haar_weight))

    per_member = places // members
    sent = latent.reshape(per_member, members, width).transpose(1, 0, 2)
    gathered = lax.all_to_all(sent, "tm", split_axis=0, concat_axis=0, tiled=True)
    encoded = pl.pallas_call(
        attention_kernel,
        out_shape=jax.ShapeDtypeStruct((members, per_member * width), BF16),
        in_specs=vmem(3),
        out_specs=vmem(1)[0],
        cost_estimate=cost(10**9, 4 * 10**6),
        compiler_params=params(),
        name="attention",
    )(gathered.reshape(members, per_member * width), query_weight, key_weight)
    returned = lax.all_to_all(
        encoded.reshape(members, per_member, width), "tm", split_axis=0, concat_axis=0, tiled=True
    )
    return returned.transpose(1, 0, 2).reshape(frames // 2, rows // 2, columns // 2, width)


def solution(mesh):
    in_specs = (
        P(("groups", "tm"), "height", None, None),
        P(),
        P(None, None, "height", None),
        P(),
        P(),
        P(),
        P(),
    )
    out_specs = P(("groups", "tm"), "height", None, None)

    return jax.shard_map(body, mesh=mesh, in_specs=in_specs, out_specs=out_specs, check_vma=False)
```

```python
import jax
import jax.numpy as jnp
from jax import lax
from jax.experimental import pallas as pl
from jax.experimental.pallas import tpu as pltpu
from jax.sharding import PartitionSpec as P


HEAD_DIM = 64
CORES = 2

epsilon = 1e-06
inv_root = 0.7071067811865476

F32 = jnp.float32
BF16 = jnp.bfloat16


def dot(a, b):
    return jnp.dot(a, b, preferred_element_type=F32)


def vmem(count):
    return [pl.BlockSpec(memory_space=pltpu.VMEM) for _ in range(count)]


def params(mib=20):
    return pltpu.CompilerParams(vmem_limit_bytes=mib * 2**20)


def cost(flops, nbytes):
    return pl.CostEstimate(flops=flops, bytes_accessed=nbytes, transcendentals=0)


def hold_kernel(video_ref, gain_ref, video_held_ref, gain_held_ref, sems):
    moves = [(video_ref, video_held_ref), (gain_ref, gain_held_ref)]
    started = [pltpu.make_async_copy(src, dst, sems.at[i]) for i, (src, dst) in enumerate(moves)]
    for copy in started:
        copy.start()
    for copy in started:
        copy.wait()


def edges_kernel(earlier_ref, video_ref, first_ref, last_ref):
    frames, rows = video_ref.shape[:2]
    for i, ref in enumerate((earlier_ref, video_ref)):
        for frame in range(frames):
            first_ref[i * frames + frame] = ref[frame, 0]
            last_ref[i * frames + frame] = ref[frame, rows - 1]


def far(x):
    return pltpu.with_memory_space_constraint(x, pltpu.HBM)


def prepare_kernel(earlier_ref, video_ref, above_ref, below_ref, gain_ref, windows_ref, ordered_ref):
    frames, rows, columns, _ = video_ref.shape
    half = columns // 2
    place = lax.broadcasted_iota(jnp.int32, (3 * columns, columns), 0)
    source = lax.broadcasted_iota(jnp.int32, (3 * columns, columns), 1)
    tap, within = place // columns, place % columns
    wanted = 2 * (within % half) + within // half + tap - 1
    pick = (source == wanted).astype(F32).astype(BF16)
    gain = gain_ref[...]
    for frame in range(2 * frames):
        for row in range(rows + 2):
            if row == 0:
                block = above_ref[frame]
            elif row == rows + 1:
                block = below_ref[frame]
            elif frame < frames:
                block = earlier_ref[frame, row - 1]
            else:
                block = video_ref[frame - frames, row - 1]
                ordered_ref[frame - frames, row - 1] = dot(pick[columns : 2 * columns], block).astype(BF16)
            values = block.astype(F32)
            square = jnp.mean(values * values, axis=-1, keepdims=True)
            normed = values * lax.rsqrt(square + epsilon) * gain
            acted = (normed * jax.nn.sigmoid(normed)).astype(BF16)
            moved = dot(pick, acted).astype(BF16)
            for t in range(3):
                windows_ref[t, frame, row] = moved[t * columns : (t + 1) * columns]


def haar_rows(values, rows, half):
    out = []
    for pair in range(rows // 2):
        blocks = [
            values[f][((2 * pair + r) * 2 + c) * half : ((2 * pair + r) * 2 + c + 1) * half]
            for f in range(2)
            for r in range(2)
            for c in range(2)
        ]
        for step in (4, 2, 1):
            split = list(blocks)
            for i in range(8):
                if not i & step:
                    split[i] = (blocks[i] + blocks[i + step]) * inv_root
                    split[i + step] = (blocks[i] - blocks[i + step]) * inv_root
            blocks = split
        out.append(jnp.concatenate([b.astype(BF16) for b in blocks], axis=1))
    return jnp.concatenate(out, axis=0)


def latent_kernel(
    core_ref, own_ref, other_ref, windows_ref, video_ref, temporal_far_ref, haar_far_ref, latent_ref, temporal_ref, haar_ref, sems
):
    frames, rows, columns, channels = video_ref.shape
    chips = own_ref.shape[0]
    temporal_copy = pltpu.make_async_copy(temporal_far_ref, temporal_ref, sems.at[0])
    haar_copy = pltpu.make_async_copy(haar_far_ref, haar_ref, sems.at[1])
    temporal_copy.start()
    haar_copy.start()
    first = core_ref[0] == 0
    taps = []
    for tap in range(9):
        parts = []
        for chip in range(chips):
            own, other = own_ref[chip, tap], other_ref[chip, tap]
            parts += [jnp.where(first, own, other), jnp.where(first, other, own)]
        taps.append(jnp.concatenate(parts, axis=0))
    spatial = []
    for frame in range(2 * frames):
        total = None
        for tap in range(9):
            a, b = tap // 3, tap % 3
            window = windows_ref[b, frame, a : a + rows].reshape(rows * columns, channels)
            term = dot(window, taps[tap])
            total = term if total is None else total + term
        spatial.append(total.astype(BF16))
    temporal_copy.wait()
    merged = []
    for frame in range(frames):
        total = video_ref[frame].reshape(rows * columns, channels).astype(F32)
        for tap in range(3):
            total = total + dot(spatial[frame + tap], temporal_ref[tap])
        merged.append(total.astype(BF16).astype(F32))
    bands = haar_rows(merged, rows, columns // 2)
    haar_copy.wait()
    latent_ref[...] = dot(bands, haar_ref[...]).astype(BF16)


def attention_kernel(latent_ref, query_ref, key_ref, out_ref):
    frames = latent_ref.shape[0]
    width = query_ref.shape[0]
    places = latent_ref.shape[1] // width
    rows = places * frames
    latent = jnp.concatenate([latent_ref[:, p * width : (p + 1) * width] for p in range(places)], axis=0)
    queries = dot(latent, query_ref[...]).astype(BF16)
    keys = dot(latent, key_ref[...]).astype(BF16)
    at = lax.broadcasted_iota(jnp.int32, (rows, rows), 0)
    to = lax.broadcasted_iota(jnp.int32, (rows, rows), 1)
    allowed = (at // frames == to // frames) & (to <= at)
    pair = 2 * HEAD_DIM
    lane = lax.broadcasted_iota(jnp.int32, (rows, pair), 1)
    sides = [(lane // HEAD_DIM == i).astype(F32).astype(BF16) for i in range(2)]
    starts = range(0, width, pair)
    scores = []
    for start in starts:
        q, k = queries[:, start : start + pair], keys[:, start : start + pair]
        for side in sides:
            score = lax.dot_general(q, k * side, (((1,), (1,)), ((), ())), preferred_element_type=F32)
            scores.append(jnp.where(allowed, score * HEAD_DIM ** (-0.5), -1e30))
    scores = jnp.concatenate(scores, axis=0)
    weights = jnp.exp(scores - jnp.max(scores, axis=-1, keepdims=True))
    probs = (weights / jnp.sum(weights, axis=-1, keepdims=True)).astype(BF16)
    pieces = []
    for i, start in enumerate(starts):
        v = latent[:, start : start + pair]
        mixed = None
        for j, side in enumerate(sides):
            term = dot(probs[(2 * i + j) * rows : (2 * i + j + 1) * rows], v * side)
            mixed = term if mixed is None else mixed + term
        pieces.append((v.astype(F32) + mixed.astype(BF16).astype(F32)).astype(BF16))
    encoded = jnp.concatenate(pieces, axis=1)
    for p in range(places):
        out_ref[:, p * width : (p + 1) * width] = encoded[p * frames : (p + 1) * frames]


def body(video, norm_gain, spatial_weight, temporal_weight, haar_weight, query_weight, key_weight):
    frames, rows, columns, channels = video.shape
    outward = spatial_weight.shape[3]
    width = haar_weight.shape[1]
    height = lax.axis_size("height")
    members = lax.axis_size("tm")
    chips = height // CORES
    slice_depth = spatial_weight.shape[2]

    earlier = lax.ppermute(video, "tm", [(i, i + 1) for i in range(members - 1)])

    hold = pl.pallas_call(
        hold_kernel,
        out_shape=(
            jax.ShapeDtypeStruct(video.shape, BF16),
            jax.ShapeDtypeStruct((1, channels), F32),
        ),
        in_specs=[pl.BlockSpec(memory_space=pl.ANY)] * 2,
        out_specs=tuple(vmem(2)),
        scratch_shapes=[pltpu.SemaphoreType.DMA((2,))],
        cost_estimate=cost(10**6, 10**6),
        compiler_params=params(),
        name="hold",
    )
    held, gain = hold(far(video), far(norm_gain.reshape(1, channels)))

    slices = spatial_weight.reshape(9, slice_depth, outward)
    same_core = [[c + CORES * i for i in range(chips)] for c in range(CORES)]
    copies = jnp.broadcast_to(slices, (chips, *slices.shape))
    own = lax.all_to_all(
        copies, "height", split_axis=0, concat_axis=0, axis_index_groups=same_core, tiled=True
    )

    rims = jax.ShapeDtypeStruct((2 * frames, columns, channels), BF16)
    trim = pl.pallas_call(
        edges_kernel,
        out_shape=(rims, rims),
        in_specs=vmem(2),
        out_specs=tuple(vmem(2)),
        cost_estimate=cost(10**6, 10**6),
        compiler_params=params(),
        name="edges",
    )
    first, last = trim(earlier, held)
    above = lax.ppermute(last, "height", [(i, i + 1) for i in range(height - 1)])
    below = lax.ppermute(first, "height", [(i + 1, i) for i in range(height - 1)])
    windows, ordered = pl.pallas_call(
        prepare_kernel,
        out_shape=(
            jax.ShapeDtypeStruct((3, 2 * frames, rows + 2, columns, channels), BF16),
            jax.ShapeDtypeStruct(video.shape, BF16),
        ),
        in_specs=vmem(5),
        out_specs=tuple(vmem(2)),
        cost_estimate=cost(10**9, 4 * 10**6),
        compiler_params=params(),
        name="prepare",
    )(earlier, held, above, below, gain)

    other = lax.ppermute(own, "height", [(i, i ^ 1) for i in range(height)])
    core = (lax.axis_index("height") % CORES).astype(jnp.int32).reshape(1)
    places = (rows // 2) * (columns // 2)
    latent = pl.pallas_call(
        latent_kernel,
        out_shape=jax.ShapeDtypeStruct((places, width), BF16),
        in_specs=[pl.BlockSpec(memory_space=pltpu.SMEM)] + vmem(4) + [pl.BlockSpec(memory_space=pl.ANY)] * 2,
        out_specs=vmem(1)[0],
        scratch_shapes=[
            pltpu.VMEM(temporal_weight.shape, BF16),
            pltpu.VMEM(haar_weight.shape, BF16),
            pltpu.SemaphoreType.DMA((2,)),
        ],
        cost_estimate=cost(4 * 10**9, 8 * 10**6),
        compiler_params=params(),
        name="latent",
    )(core, own, other, windows, ordered, far(temporal_weight), far(haar_weight))

    per_member = places // members
    sent = latent.reshape(per_member, members, width).transpose(1, 0, 2)
    gathered = lax.all_to_all(sent, "tm", split_axis=0, concat_axis=0, tiled=True)
    encoded = pl.pallas_call(
        attention_kernel,
        out_shape=jax.ShapeDtypeStruct((members, per_member * width), BF16),
        in_specs=vmem(3),
        out_specs=vmem(1)[0],
        cost_estimate=cost(10**9, 4 * 10**6),
        compiler_params=params(),
        name="attention",
    )(gathered.reshape(members, per_member * width), query_weight, key_weight)
    returned = lax.all_to_all(
        encoded.reshape(members, per_member, width), "tm", split_axis=0, concat_axis=0, tiled=True
    )
    return returned.transpose(1, 0, 2).reshape(frames // 2, rows // 2, columns // 2, width)


def solution(mesh):
    in_specs = (
        P(("groups", "tm"), "height", None, None),
        P(),
        P(None, None, "height", None),
        P(),
        P(),
        P(),
        P(),
    )
    out_specs = P(("groups", "tm"), "height", None, None)

    return jax.shard_map(body, mesh=mesh, in_specs=in_specs, out_specs=out_specs, check_vma=False)
```

```python
import jax
import jax.numpy as jnp
from jax import lax
from jax.experimental import pallas as pl
from jax.experimental.pallas import tpu as pltpu
from jax.sharding import PartitionSpec as P


HEAD_DIM = 64
CORES = 2

epsilon = 1e-06
inv_root = 0.7071067811865476

F32 = jnp.float32
BF16 = jnp.bfloat16


def dot(a, b):
    return jnp.dot(a, b, preferred_element_type=F32)


def vmem(count):
    return [pl.BlockSpec(memory_space=pltpu.VMEM) for _ in range(count)]


def params(mib=20):
    return pltpu.CompilerParams(vmem_limit_bytes=mib * 2**20)


def cost(flops, nbytes):
    return pl.CostEstimate(flops=flops, bytes_accessed=nbytes, transcendentals=0)


def hold_kernel(slices_ref, video_ref, gain_ref, slices_held_ref, video_held_ref, gain_held_ref, sems):
    moves = [(slices_ref, slices_held_ref), (video_ref, video_held_ref), (gain_ref, gain_held_ref)]
    started = [pltpu.make_async_copy(src, dst, sems.at[i]) for i, (src, dst) in enumerate(moves)]
    for copy in started:
        copy.start()
    for copy in started:
        copy.wait()


def stack_kernel(first_ref, second_ref, both_ref):
    middle = both_ref.shape[0] // 2
    both_ref[:middle] = first_ref[...].reshape(both_ref[:middle].shape)
    both_ref[middle:] = second_ref[...].reshape(both_ref[middle:].shape)


def stacked(first, second, count):
    return pl.pallas_call(
        stack_kernel,
        out_shape=jax.ShapeDtypeStruct((count, *first.shape[-3:]), BF16),
        in_specs=vmem(2),
        out_specs=vmem(1)[0],
        cost_estimate=cost(10**6, 10**6),
        compiler_params=params(),
        name="stack",
    )(first, second)


def edges_kernel(earlier_ref, video_ref, first_ref, last_ref):
    frames, rows = video_ref.shape[:2]
    for i, ref in enumerate((earlier_ref, video_ref)):
        for frame in range(frames):
            first_ref[i * frames + frame] = ref[frame, 0]
            last_ref[i * frames + frame] = ref[frame, rows - 1]


def far(x):
    return pltpu.with_memory_space_constraint(x, pltpu.HBM)


def prepare_kernel(earlier_ref, video_ref, above_ref, below_ref, gain_ref, windows_ref, ordered_ref):
    frames, rows, columns, _ = video_ref.shape
    half = columns // 2
    place = lax.broadcasted_iota(jnp.int32, (3 * columns, columns), 0)
    source = lax.broadcasted_iota(jnp.int32, (3 * columns, columns), 1)
    tap, within = place // columns, place % columns
    wanted = 2 * (within % half) + within // half + tap - 1
    pick = (source == wanted).astype(F32).astype(BF16)
    gain = gain_ref[...]
    for frame in range(2 * frames):
        for row in range(rows + 2):
            if row == 0:
                block = above_ref[frame]
            elif row == rows + 1:
                block = below_ref[frame]
            elif frame < frames:
                block = earlier_ref[frame, row - 1]
            else:
                block = video_ref[frame - frames, row - 1]
                ordered_ref[frame - frames, row - 1] = dot(pick[columns : 2 * columns], block).astype(BF16)
            values = block.astype(F32)
            square = jnp.mean(values * values, axis=-1, keepdims=True)
            normed = values * lax.rsqrt(square + epsilon) * gain
            acted = (normed * jax.nn.sigmoid(normed)).astype(BF16)
            moved = dot(pick, acted).astype(BF16)
            for t in range(3):
                windows_ref[t, frame, row] = moved[t * columns : (t + 1) * columns]


def haar_rows(values, rows, half):
    out = []
    for pair in range(rows // 2):
        blocks = [
            values[f][((2 * pair + r) * 2 + c) * half : ((2 * pair + r) * 2 + c + 1) * half]
            for f in range(2)
            for r in range(2)
            for c in range(2)
        ]
        for step in (4, 2, 1):
            split = list(blocks)
            for i in range(8):
                if not i & step:
                    split[i] = (blocks[i] + blocks[i + step]) * inv_root
                    split[i + step] = (blocks[i] - blocks[i + step]) * inv_root
            blocks = split
        out.append(jnp.concatenate([b.astype(BF16) for b in blocks], axis=1))
    return jnp.concatenate(out, axis=0)


def latent_kernel(
    at_ref, own_ref, other_ref, windows_ref, video_ref, temporal_far_ref, haar_far_ref, latent_ref, temporal_ref, haar_ref, sems
):
    frames, rows, columns, channels = video_ref.shape
    chips = own_ref.shape[0]
    temporal_copy = pltpu.make_async_copy(temporal_far_ref, temporal_ref, sems.at[0])
    haar_copy = pltpu.make_async_copy(haar_far_ref, haar_ref, sems.at[1])
    temporal_copy.start()
    haar_copy.start()
    first = at_ref[1] == 0
    taps = []
    for tap in range(9):
        parts = []
        for chip in range(chips):
            apart = lax.bitwise_xor(jnp.int32(chip), at_ref[0])
            slot = lax.bitwise_xor(apart, lax.shift_right_logical(apart, jnp.int32(1)))
            own, other = own_ref[slot, tap], other_ref[slot, tap]
            parts += [jnp.where(first, own, other), jnp.where(first, other, own)]
        taps.append(jnp.concatenate(parts, axis=0))
    spatial = []
    for frame in range(2 * frames):
        total = None
        for tap in range(9):
            a, b = tap // 3, tap % 3
            window = windows_ref[b, frame, a : a + rows].reshape(rows * columns, channels)
            term = dot(window, taps[tap])
            total = term if total is None else total + term
        spatial.append(total.astype(BF16))
    temporal_copy.wait()
    merged = []
    for frame in range(frames):
        total = video_ref[frame].reshape(rows * columns, channels).astype(F32)
        for tap in range(3):
            total = total + dot(spatial[frame + tap], temporal_ref[tap])
        merged.append(total.astype(BF16).astype(F32))
    bands = haar_rows(merged, rows, columns // 2)
    haar_copy.wait()
    latent_ref[...] = dot(bands, haar_ref[...]).astype(BF16)


def attention_kernel(latent_ref, query_ref, key_ref, out_ref):
    frames = latent_ref.shape[0]
    width = query_ref.shape[0]
    places = latent_ref.shape[1] // width
    rows = places * frames
    latent = jnp.concatenate([latent_ref[:, p * width : (p + 1) * width] for p in range(places)], axis=0)
    queries = dot(latent, query_ref[...]).astype(BF16)
    keys = dot(latent, key_ref[...]).astype(BF16)
    at = lax.broadcasted_iota(jnp.int32, (rows, rows), 0)
    to = lax.broadcasted_iota(jnp.int32, (rows, rows), 1)
    allowed = (at // frames == to // frames) & (to <= at)
    pair = 2 * HEAD_DIM
    lane = lax.broadcasted_iota(jnp.int32, (rows, pair), 1)
    sides = [(lane // HEAD_DIM == i).astype(F32).astype(BF16) for i in range(2)]
    starts = range(0, width, pair)
    scores = []
    for start in starts:
        q, k = queries[:, start : start + pair], keys[:, start : start + pair]
        for side in sides:
            score = lax.dot_general(q, k * side, (((1,), (1,)), ((), ())), preferred_element_type=F32)
            scores.append(jnp.where(allowed, score * HEAD_DIM ** (-0.5), -1e30))
    scores = jnp.concatenate(scores, axis=0)
    weights = jnp.exp(scores - jnp.max(scores, axis=-1, keepdims=True))
    probs = (weights / jnp.sum(weights, axis=-1, keepdims=True)).astype(BF16)
    pieces = []
    for i, start in enumerate(starts):
        v = latent[:, start : start + pair]
        mixed = None
        for j, side in enumerate(sides):
            term = dot(probs[(2 * i + j) * rows : (2 * i + j + 1) * rows], v * side)
            mixed = term if mixed is None else mixed + term
        pieces.append((v.astype(F32) + mixed.astype(BF16).astype(F32)).astype(BF16))
    encoded = jnp.concatenate(pieces, axis=1)
    for p in range(places):
        out_ref[:, p * width : (p + 1) * width] = encoded[p * frames : (p + 1) * frames]


def body(video, norm_gain, spatial_weight, temporal_weight, haar_weight, query_weight, key_weight):
    frames, rows, columns, channels = video.shape
    outward = spatial_weight.shape[3]
    width = haar_weight.shape[1]
    height = lax.axis_size("height")
    members = lax.axis_size("tm")
    chips = height // CORES
    slice_depth = spatial_weight.shape[2]

    earlier = lax.ppermute(video, "tm", [(i, i + 1) for i in range(members - 1)])

    if chips != 4:
        raise ValueError("four chips")
    slices = spatial_weight.reshape(9, slice_depth, outward)

    def swapped(x, apart):
        pairs = [(CORES * i + c, CORES * (i ^ apart) + c) for i in range(chips) for c in range(CORES)]
        return lax.ppermute(x, "height", pairs)

    hold = pl.pallas_call(
        hold_kernel,
        out_shape=(
            jax.ShapeDtypeStruct(slices.shape, BF16),
            jax.ShapeDtypeStruct(video.shape, BF16),
            jax.ShapeDtypeStruct((1, channels), F32),
        ),
        in_specs=[pl.BlockSpec(memory_space=pl.ANY)] * 3,
        out_specs=tuple(vmem(3)),
        scratch_shapes=[pltpu.SemaphoreType.DMA((3,))],
        cost_estimate=cost(10**6, 10**6),
        compiler_params=params(),
        name="hold",
    )
    near = swapped(slices, 1)
    slices_held, held, gain = hold(far(slices), far(video), far(norm_gain.reshape(1, channels)))
    pair = stacked(slices_held, near, 2)
    across = swapped(pair, 3)
    own = stacked(pair, across, 4)

    rims = jax.ShapeDtypeStruct((2 * frames, columns, channels), BF16)
    trim = pl.pallas_call(
        edges_kernel,
        out_shape=(rims, rims),
        in_specs=vmem(2),
        out_specs=tuple(vmem(2)),
        cost_estimate=cost(10**6, 10**6),
        compiler_params=params(),
        name="edges",
    )
    first, last = trim(earlier, held)
    above = lax.ppermute(last, "height", [(i, i + 1) for i in range(height - 1)])
    below = lax.ppermute(first, "height", [(i + 1, i) for i in range(height - 1)])
    windows, ordered = pl.pallas_call(
        prepare_kernel,
        out_shape=(
            jax.ShapeDtypeStruct((3, 2 * frames, rows + 2, columns, channels), BF16),
            jax.ShapeDtypeStruct(video.shape, BF16),
        ),
        in_specs=vmem(5),
        out_specs=tuple(vmem(2)),
        cost_estimate=cost(10**9, 4 * 10**6),
        compiler_params=params(),
        name="prepare",
    )(earlier, held, above, below, gain)

    other = lax.ppermute(own, "height", [(i, i ^ 1) for i in range(height)])
    index = lax.axis_index("height").astype(jnp.int32)
    at = jnp.stack([index // CORES, index % CORES])
    places = (rows // 2) * (columns // 2)
    latent = pl.pallas_call(
        latent_kernel,
        out_shape=jax.ShapeDtypeStruct((places, width), BF16),
        in_specs=[pl.BlockSpec(memory_space=pltpu.SMEM)] + vmem(4) + [pl.BlockSpec(memory_space=pl.ANY)] * 2,
        out_specs=vmem(1)[0],
        scratch_shapes=[
            pltpu.VMEM(temporal_weight.shape, BF16),
            pltpu.VMEM(haar_weight.shape, BF16),
            pltpu.SemaphoreType.DMA((2,)),
        ],
        cost_estimate=cost(4 * 10**9, 8 * 10**6),
        compiler_params=params(),
        name="latent",
    )(at, own, other, windows, ordered, far(temporal_weight), far(haar_weight))

    per_member = places // members
    sent = latent.reshape(per_member, members, width).transpose(1, 0, 2)
    gathered = lax.all_to_all(sent, "tm", split_axis=0, concat_axis=0, tiled=True)
    encoded = pl.pallas_call(
        attention_kernel,
        out_shape=jax.ShapeDtypeStruct((members, per_member * width), BF16),
        in_specs=vmem(3),
        out_specs=vmem(1)[0],
        cost_estimate=cost(10**9, 4 * 10**6),
        compiler_params=params(),
        name="attention",
    )(gathered.reshape(members, per_member * width), query_weight, key_weight)
    returned = lax.all_to_all(
        encoded.reshape(members, per_member, width), "tm", split_axis=0, concat_axis=0, tiled=True
    )
    return returned.transpose(1, 0, 2).reshape(frames // 2, rows // 2, columns // 2, width)


def solution(mesh):
    in_specs = (
        P(("groups", "tm"), "height", None, None),
        P(),
        P(None, None, "height", None),
        P(),
        P(),
        P(),
        P(),
    )
    out_specs = P(("groups", "tm"), "height", None, None)

    return jax.shard_map(body, mesh=mesh, in_specs=in_specs, out_specs=out_specs, check_vma=False)
```

```python
import jax
import jax.numpy as jnp
from jax import lax
from jax.experimental import pallas as pl
from jax.experimental.pallas import tpu as pltpu
from jax.sharding import PartitionSpec as P


HEAD_DIM = 64
CORES = 2

epsilon = 1e-06
inv_root = 0.7071067811865476

F32 = jnp.float32
BF16 = jnp.bfloat16


def dot(a, b):
    return jnp.dot(a, b, preferred_element_type=F32)


def vmem(count):
    return [pl.BlockSpec(memory_space=pltpu.VMEM) for _ in range(count)]


def params(mib=20):
    return pltpu.CompilerParams(vmem_limit_bytes=mib * 2**20)


def cost(flops, nbytes):
    return pl.CostEstimate(flops=flops, bytes_accessed=nbytes, transcendentals=0)


def hold_kernel(video_ref, gain_ref, video_held_ref, gain_held_ref, sems):
    moves = [(video_ref, video_held_ref), (gain_ref, gain_held_ref)]
    started = [pltpu.make_async_copy(src, dst, sems.at[i]) for i, (src, dst) in enumerate(moves)]
    for copy in started:
        copy.start()
    for copy in started:
        copy.wait()


def edges_kernel(earlier_ref, video_ref, first_ref, last_ref):
    frames, rows = video_ref.shape[:2]
    for i, ref in enumerate((earlier_ref, video_ref)):
        for frame in range(frames):
            first_ref[i * frames + frame] = ref[frame, 0]
            last_ref[i * frames + frame] = ref[frame, rows - 1]


def far(x):
    return pltpu.with_memory_space_constraint(x, pltpu.HBM)


def prepare_kernel(earlier_ref, video_ref, above_ref, below_ref, gain_ref, windows_ref, ordered_ref):
    frames, rows, columns, _ = video_ref.shape
    half = columns // 2
    place = lax.broadcasted_iota(jnp.int32, (3 * columns, columns), 0)
    source = lax.broadcasted_iota(jnp.int32, (3 * columns, columns), 1)
    tap, within = place // columns, place % columns
    wanted = 2 * (within % half) + within // half + tap - 1
    pick = (source == wanted).astype(F32).astype(BF16)
    gain = gain_ref[...]
    for frame in range(2 * frames):
        for row in range(rows + 2):
            if row == 0:
                block = above_ref[frame]
            elif row == rows + 1:
                block = below_ref[frame]
            elif frame < frames:
                block = earlier_ref[frame, row - 1]
            else:
                block = video_ref[frame - frames, row - 1]
                ordered_ref[frame - frames, row - 1] = dot(pick[columns : 2 * columns], block).astype(BF16)
            values = block.astype(F32)
            square = jnp.mean(values * values, axis=-1, keepdims=True)
            normed = values * lax.rsqrt(square + epsilon) * gain
            acted = (normed * jax.nn.sigmoid(normed)).astype(BF16)
            moved = dot(pick, acted).astype(BF16)
            for t in range(3):
                windows_ref[t, frame, row] = moved[t * columns : (t + 1) * columns]


def haar_rows(values, rows, half):
    out = []
    for pair in range(rows // 2):
        blocks = [
            values[f][((2 * pair + r) * 2 + c) * half : ((2 * pair + r) * 2 + c + 1) * half]
            for f in range(2)
            for r in range(2)
            for c in range(2)
        ]
        for step in (4, 2, 1):
            split = list(blocks)
            for i in range(8):
                if not i & step:
                    split[i] = (blocks[i] + blocks[i + step]) * inv_root
                    split[i + step] = (blocks[i] - blocks[i + step]) * inv_root
            blocks = split
        out.append(jnp.concatenate([b.astype(BF16) for b in blocks], axis=1))
    return jnp.concatenate(out, axis=0)


def latent_kernel(
    core_ref, own_ref, other_ref, windows_ref, video_ref, temporal_far_ref, haar_far_ref, latent_ref, temporal_ref, haar_ref, sems
):
    frames, rows, columns, channels = video_ref.shape
    chips = own_ref.shape[0]
    temporal_copy = pltpu.make_async_copy(temporal_far_ref, temporal_ref, sems.at[0])
    haar_copy = pltpu.make_async_copy(haar_far_ref, haar_ref, sems.at[1])
    temporal_copy.start()
    haar_copy.start()
    first = core_ref[0] == 0
    taps = []
    for tap in range(9):
        parts = []
        for chip in range(chips):
            back = chips - 1 - chip
            parts += [
                jnp.where(first, own_ref[chip, tap], other_ref[chip, tap]),
                jnp.where(first, other_ref[back, tap], own_ref[back, tap]),
            ]
        taps.append(jnp.concatenate(parts, axis=0))
    spatial = []
    for frame in range(2 * frames):
        total = None
        for tap in range(9):
            a, b = tap // 3, tap % 3
            window = windows_ref[b, frame, a : a + rows].reshape(rows * columns, channels)
            term = dot(window, taps[tap])
            total = term if total is None else total + term
        spatial.append(total.astype(BF16))
    temporal_copy.wait()
    merged = []
    for frame in range(frames):
        total = video_ref[frame].reshape(rows * columns, channels).astype(F32)
        for tap in range(3):
            total = total + dot(spatial[frame + tap], temporal_ref[tap])
        merged.append(total.astype(BF16).astype(F32))
    bands = haar_rows(merged, rows, columns // 2)
    haar_copy.wait()
    latent_ref[...] = dot(bands, haar_ref[...]).astype(BF16)


def attention_kernel(latent_ref, query_ref, key_ref, out_ref):
    frames = latent_ref.shape[0]
    width = query_ref.shape[0]
    places = latent_ref.shape[1] // width
    rows = places * frames
    latent = jnp.concatenate([latent_ref[:, p * width : (p + 1) * width] for p in range(places)], axis=0)
    queries = dot(latent, query_ref[...]).astype(BF16)
    keys = dot(latent, key_ref[...]).astype(BF16)
    at = lax.broadcasted_iota(jnp.int32, (rows, rows), 0)
    to = lax.broadcasted_iota(jnp.int32, (rows, rows), 1)
    allowed = (at // frames == to // frames) & (to <= at)
    pair = 2 * HEAD_DIM
    lane = lax.broadcasted_iota(jnp.int32, (rows, pair), 1)
    sides = [(lane // HEAD_DIM == i).astype(F32).astype(BF16) for i in range(2)]
    starts = range(0, width, pair)
    scores = []
    for start in starts:
        q, k = queries[:, start : start + pair], keys[:, start : start + pair]
        for side in sides:
            score = lax.dot_general(q, k * side, (((1,), (1,)), ((), ())), preferred_element_type=F32)
            scores.append(jnp.where(allowed, score * HEAD_DIM ** (-0.5), -1e30))
    scores = jnp.concatenate(scores, axis=0)
    weights = jnp.exp(scores - jnp.max(scores, axis=-1, keepdims=True))
    probs = (weights / jnp.sum(weights, axis=-1, keepdims=True)).astype(BF16)
    pieces = []
    for i, start in enumerate(starts):
        v = latent[:, start : start + pair]
        mixed = None
        for j, side in enumerate(sides):
            term = dot(probs[(2 * i + j) * rows : (2 * i + j + 1) * rows], v * side)
            mixed = term if mixed is None else mixed + term
        pieces.append((v.astype(F32) + mixed.astype(BF16).astype(F32)).astype(BF16))
    encoded = jnp.concatenate(pieces, axis=1)
    for p in range(places):
        out_ref[:, p * width : (p + 1) * width] = encoded[p * frames : (p + 1) * frames]


def body(video, norm_gain, spatial_weight, temporal_weight, haar_weight, query_weight, key_weight):
    frames, rows, columns, channels = video.shape
    outward = spatial_weight.shape[3]
    width = haar_weight.shape[1]
    height = lax.axis_size("height")
    members = lax.axis_size("tm")
    chips = height // CORES
    slice_depth = spatial_weight.shape[2]

    earlier = lax.ppermute(video, "tm", [(i, i + 1) for i in range(members - 1)])

    hold = pl.pallas_call(
        hold_kernel,
        out_shape=(
            jax.ShapeDtypeStruct(video.shape, BF16),
            jax.ShapeDtypeStruct((1, channels), F32),
        ),
        in_specs=[pl.BlockSpec(memory_space=pl.ANY)] * 2,
        out_specs=tuple(vmem(2)),
        scratch_shapes=[pltpu.SemaphoreType.DMA((2,))],
        cost_estimate=cost(10**6, 10**6),
        compiler_params=params(),
        name="hold",
    )
    held, gain = hold(far(video), far(norm_gain.reshape(1, channels)))

    slices = spatial_weight.reshape(9, slice_depth, outward)
    same_core = [[c + CORES * i for i in range(chips)] for c in range(CORES)]
    same_core[1].reverse()
    copies = jnp.broadcast_to(slices, (chips, *slices.shape))
    own = lax.all_to_all(
        copies, "height", split_axis=0, concat_axis=0, axis_index_groups=same_core, tiled=True
    )

    rims = jax.ShapeDtypeStruct((2 * frames, columns, channels), BF16)
    trim = pl.pallas_call(
        edges_kernel,
        out_shape=(rims, rims),
        in_specs=vmem(2),
        out_specs=tuple(vmem(2)),
        cost_estimate=cost(10**6, 10**6),
        compiler_params=params(),
        name="edges",
    )
    first, last = trim(earlier, held)
    above = lax.ppermute(last, "height", [(i, i + 1) for i in range(height - 1)])
    below = lax.ppermute(first, "height", [(i + 1, i) for i in range(height - 1)])
    windows, ordered = pl.pallas_call(
        prepare_kernel,
        out_shape=(
            jax.ShapeDtypeStruct((3, 2 * frames, rows + 2, columns, channels), BF16),
            jax.ShapeDtypeStruct(video.shape, BF16),
        ),
        in_specs=vmem(5),
        out_specs=tuple(vmem(2)),
        cost_estimate=cost(10**9, 4 * 10**6),
        compiler_params=params(),
        name="prepare",
    )(earlier, held, above, below, gain)

    other = lax.ppermute(own, "height", [(i, i ^ 1) for i in range(height)])
    core = (lax.axis_index("height") % CORES).astype(jnp.int32).reshape(1)
    places = (rows // 2) * (columns // 2)
    latent = pl.pallas_call(
        latent_kernel,
        out_shape=jax.ShapeDtypeStruct((places, width), BF16),
        in_specs=[pl.BlockSpec(memory_space=pltpu.SMEM)] + vmem(4) + [pl.BlockSpec(memory_space=pl.ANY)] * 2,
        out_specs=vmem(1)[0],
        scratch_shapes=[
            pltpu.VMEM(temporal_weight.shape, BF16),
            pltpu.VMEM(haar_weight.shape, BF16),
            pltpu.SemaphoreType.DMA((2,)),
        ],
        cost_estimate=cost(4 * 10**9, 8 * 10**6),
        compiler_params=params(),
        name="latent",
    )(core, own, other, windows, ordered, far(temporal_weight), far(haar_weight))

    per_member = places // members
    sent = latent.reshape(per_member, members, width).transpose(1, 0, 2)
    gathered = lax.all_to_all(sent, "tm", split_axis=0, concat_axis=0, tiled=True)
    encoded = pl.pallas_call(
        attention_kernel,
        out_shape=jax.ShapeDtypeStruct((members, per_member * width), BF16),
        in_specs=vmem(3),
        out_specs=vmem(1)[0],
        cost_estimate=cost(10**9, 4 * 10**6),
        compiler_params=params(),
        name="attention",
    )(gathered.reshape(members, per_member * width), query_weight, key_weight)
    returned = lax.all_to_all(
        encoded.reshape(members, per_member, width), "tm", split_axis=0, concat_axis=0, tiled=True
    )
    return returned.transpose(1, 0, 2).reshape(frames // 2, rows // 2, columns // 2, width)


def solution(mesh):
    in_specs = (
        P(("groups", "tm"), "height", None, None),
        P(),
        P(None, None, "height", None),
        P(),
        P(),
        P(),
        P(),
    )
    out_specs = P(("groups", "tm"), "height", None, None)

    return jax.shard_map(body, mesh=mesh, in_specs=in_specs, out_specs=out_specs, check_vma=False)
```

```python
import jax
import jax.numpy as jnp
from jax import lax
from jax.experimental import pallas as pl
from jax.experimental.pallas import tpu as pltpu
from jax.sharding import PartitionSpec as P


HEAD_DIM = 64
CORES = 2

epsilon = 1e-06
inv_root = 0.7071067811865476

F32 = jnp.float32
BF16 = jnp.bfloat16


def dot(a, b):
    return jnp.dot(a, b, preferred_element_type=F32)


def vmem(count):
    return [pl.BlockSpec(memory_space=pltpu.VMEM) for _ in range(count)]


def params(mib=20):
    return pltpu.CompilerParams(vmem_limit_bytes=mib * 2**20)


def cost(flops, nbytes):
    return pl.CostEstimate(flops=flops, bytes_accessed=nbytes, transcendentals=0)


def hold_kernel(video_ref, gain_ref, video_held_ref, gain_held_ref, sems):
    moves = [(video_ref, video_held_ref), (gain_ref, gain_held_ref)]
    started = [pltpu.make_async_copy(src, dst, sems.at[i]) for i, (src, dst) in enumerate(moves)]
    for copy in started:
        copy.start()
    for copy in started:
        copy.wait()


def edges_kernel(earlier_ref, video_ref, first_ref, last_ref):
    frames, rows = video_ref.shape[:2]
    for i, ref in enumerate((earlier_ref, video_ref)):
        for frame in range(frames):
            first_ref[i * frames + frame] = ref[frame, 0]
            last_ref[i * frames + frame] = ref[frame, rows - 1]


def far(x):
    return pltpu.with_memory_space_constraint(x, pltpu.HBM)


def prepare_kernel(earlier_ref, video_ref, above_ref, below_ref, gain_ref, windows_ref, ordered_ref):
    frames, rows, columns, _ = video_ref.shape
    half = columns // 2
    place = lax.broadcasted_iota(jnp.int32, (3 * columns, columns), 0)
    source = lax.broadcasted_iota(jnp.int32, (3 * columns, columns), 1)
    tap, within = place // columns, place % columns
    wanted = 2 * (within % half) + within // half + tap - 1
    pick = (source == wanted).astype(F32).astype(BF16)
    gain = gain_ref[...]
    for frame in range(2 * frames):
        for row in range(rows + 2):
            if row == 0:
                block = above_ref[frame]
            elif row == rows + 1:
                block = below_ref[frame]
            elif frame < frames:
                block = earlier_ref[frame, row - 1]
            else:
                block = video_ref[frame - frames, row - 1]
                ordered_ref[frame - frames, row - 1] = dot(pick[columns : 2 * columns], block).astype(BF16)
            values = block.astype(F32)
            square = jnp.mean(values * values, axis=-1, keepdims=True)
            normed = values * lax.rsqrt(square + epsilon) * gain
            acted = (normed * jax.nn.sigmoid(normed)).astype(BF16)
            moved = dot(pick, acted).astype(BF16)
            for t in range(3):
                windows_ref[t, frame, row] = moved[t * columns : (t + 1) * columns]


def haar_rows(values, rows, half):
    out = []
    for pair in range(rows // 2):
        blocks = [
            values[f][((2 * pair + r) * 2 + c) * half : ((2 * pair + r) * 2 + c + 1) * half]
            for f in range(2)
            for r in range(2)
            for c in range(2)
        ]
        for step in (4, 2, 1):
            split = list(blocks)
            for i in range(8):
                if not i & step:
                    split[i] = (blocks[i] + blocks[i + step]) * inv_root
                    split[i + step] = (blocks[i] - blocks[i + step]) * inv_root
            blocks = split
        out.append(jnp.concatenate([b.astype(BF16) for b in blocks], axis=1))
    return jnp.concatenate(out, axis=0)


def latent_kernel(
    core_ref, own_ref, other_ref, windows_ref, video_ref, temporal_far_ref, haar_far_ref, latent_ref, temporal_ref, haar_ref, sems
):
    frames, rows, columns, channels = video_ref.shape
    chips = own_ref.shape[0]
    temporal_copy = pltpu.make_async_copy(temporal_far_ref, temporal_ref, sems.at[0])
    haar_copy = pltpu.make_async_copy(haar_far_ref, haar_ref, sems.at[1])
    temporal_copy.start()
    haar_copy.start()
    first = core_ref[0] == 0
    taps = []
    for tap in range(9):
        parts = []
        for chip in range(chips):
            own, other = own_ref[chip, tap], other_ref[chip, tap]
            parts += [jnp.where(first, own, other), jnp.where(first, other, own)]
        taps.append(jnp.concatenate(parts, axis=0))
    spatial = []
    for frame in range(2 * frames):
        total = None
        for tap in range(9):
            a, b = tap // 3, tap % 3
            window = windows_ref[b, frame, a : a + rows].reshape(rows * columns, channels)
            term = dot(window, taps[tap])
            total = term if total is None else total + term
        spatial.append(total.astype(BF16))
    temporal_copy.wait()
    merged = []
    for frame in range(frames):
        total = video_ref[frame].reshape(rows * columns, channels).astype(F32)
        for tap in range(3):
            total = total + dot(spatial[frame + tap], temporal_ref[tap])
        merged.append(total.astype(BF16).astype(F32))
    bands = haar_rows(merged, rows, columns // 2)
    haar_copy.wait()
    latent_ref[...] = dot(bands, haar_ref[...]).astype(BF16)


def attention_kernel(latent_ref, query_ref, key_ref, out_ref):
    frames = latent_ref.shape[0]
    width = query_ref.shape[0]
    places = latent_ref.shape[1] // width
    rows = places * frames
    latent = jnp.concatenate([latent_ref[:, p * width : (p + 1) * width] for p in range(places)], axis=0)
    queries = dot(latent, query_ref[...]).astype(BF16)
    keys = dot(latent, key_ref[...]).astype(BF16)
    at = lax.broadcasted_iota(jnp.int32, (rows, rows), 0)
    to = lax.broadcasted_iota(jnp.int32, (rows, rows), 1)
    allowed = (at // frames == to // frames) & (to <= at)
    pair = 2 * HEAD_DIM
    lane = lax.broadcasted_iota(jnp.int32, (rows, pair), 1)
    sides = [(lane // HEAD_DIM == i).astype(F32).astype(BF16) for i in range(2)]
    starts = range(0, width, pair)
    scores = []
    for start in starts:
        q, k = queries[:, start : start + pair], keys[:, start : start + pair]
        for side in sides:
            score = lax.dot_general(q, k * side, (((1,), (1,)), ((), ())), preferred_element_type=F32)
            scores.append(jnp.where(allowed, score * HEAD_DIM ** (-0.5), -1e30))
    scores = jnp.concatenate(scores, axis=0)
    weights = jnp.exp(scores - jnp.max(scores, axis=-1, keepdims=True))
    probs = (weights / jnp.sum(weights, axis=-1, keepdims=True)).astype(BF16)
    pieces = []
    for i, start in enumerate(starts):
        v = latent[:, start : start + pair]
        mixed = None
        for j, side in enumerate(sides):
            term = dot(probs[(2 * i + j) * rows : (2 * i + j + 1) * rows], v * side)
            mixed = term if mixed is None else mixed + term
        pieces.append((v.astype(F32) + mixed.astype(BF16).astype(F32)).astype(BF16))
    encoded = jnp.concatenate(pieces, axis=1)
    for p in range(places):
        out_ref[:, p * width : (p + 1) * width] = encoded[p * frames : (p + 1) * frames]


def body(video, norm_gain, spatial_weight, temporal_weight, haar_weight, query_weight, key_weight):
    frames, rows, columns, channels = video.shape
    outward = spatial_weight.shape[3]
    width = haar_weight.shape[1]
    height = lax.axis_size("height")
    members = lax.axis_size("tm")
    chips = height // CORES
    slice_depth = spatial_weight.shape[2]

    earlier = lax.ppermute(video, "tm", [(i, i + 1) for i in range(members - 1)])

    hold = pl.pallas_call(
        hold_kernel,
        out_shape=(
            jax.ShapeDtypeStruct(video.shape, BF16),
            jax.ShapeDtypeStruct((1, channels), F32),
        ),
        in_specs=[pl.BlockSpec(memory_space=pl.ANY)] * 2,
        out_specs=tuple(vmem(2)),
        scratch_shapes=[pltpu.SemaphoreType.DMA((2,))],
        cost_estimate=cost(10**6, 10**6),
        compiler_params=params(),
        name="hold",
    )
    held, gain = hold(far(video), far(norm_gain.reshape(1, channels)))

    slices = spatial_weight.reshape(9, slice_depth, outward)
    same_core = [[c + CORES * i for i in range(chips)] for c in range(CORES)]
    copies = jnp.broadcast_to(slices, (chips, *slices.shape))
    own = lax.all_to_all(
        copies, "height", split_axis=0, concat_axis=0, axis_index_groups=same_core, tiled=True
    )

    rims = jax.ShapeDtypeStruct((2 * frames, columns, channels), BF16)
    trim = pl.pallas_call(
        edges_kernel,
        out_shape=(rims, rims),
        in_specs=vmem(2),
        out_specs=tuple(vmem(2)),
        cost_estimate=cost(10**6, 10**6),
        compiler_params=params(),
        name="edges",
    )
    first, last = trim(earlier, held)
    above = lax.ppermute(last, "height", [(i, i + 1) for i in range(height - 1)])
    below = lax.ppermute(first, "height", [(i + 1, i) for i in range(height - 1)])
    windows, ordered = pl.pallas_call(
        prepare_kernel,
        out_shape=(
            jax.ShapeDtypeStruct((3, 2 * frames, rows + 2, columns, channels), BF16),
            jax.ShapeDtypeStruct(video.shape, BF16),
        ),
        in_specs=vmem(5),
        out_specs=tuple(vmem(2)),
        cost_estimate=cost(10**9, 4 * 10**6),
        compiler_params=params(),
        name="prepare",
    )(earlier, held, above, below, gain)

    other = lax.ppermute(own, "height", [(i, i ^ 1) for i in range(height)])
    core = (lax.axis_index("height") % CORES).astype(jnp.int32).reshape(1)
    places = (rows // 2) * (columns // 2)
    latent = pl.pallas_call(
        latent_kernel,
        out_shape=jax.ShapeDtypeStruct((places, width), BF16),
        in_specs=[pl.BlockSpec(memory_space=pltpu.SMEM)] + vmem(4) + [pl.BlockSpec(memory_space=pl.ANY)] * 2,
        out_specs=vmem(1)[0],
        scratch_shapes=[
            pltpu.VMEM(temporal_weight.shape, BF16),
            pltpu.VMEM(haar_weight.shape, BF16),
            pltpu.SemaphoreType.DMA((2,)),
        ],
        cost_estimate=cost(4 * 10**9, 8 * 10**6),
        compiler_params=params(),
        name="latent",
    )(core, own, other, windows, ordered, far(temporal_weight), far(haar_weight))

    per_member = places // members
    lanes = 128
    blocks = width // lanes
    message = (per_member * blocks, lanes)
    sent = latent.reshape(per_member, members, blocks, lanes).transpose(1, 0, 2, 3).reshape(members, *message)
    gathered = lax.all_to_all(sent, "tm", split_axis=0, concat_axis=0, tiled=True)
    encoded = pl.pallas_call(
        attention_kernel,
        out_shape=jax.ShapeDtypeStruct((members, per_member * width), BF16),
        in_specs=vmem(3),
        out_specs=vmem(1)[0],
        cost_estimate=cost(10**9, 4 * 10**6),
        compiler_params=params(),
        name="attention",
    )(gathered.reshape(members, per_member * width), query_weight, key_weight)
    returned = lax.all_to_all(
        encoded.reshape(members, *message), "tm", split_axis=0, concat_axis=0, tiled=True
    )
    returned = returned.reshape(members, per_member, blocks, lanes).transpose(1, 0, 2, 3)
    return returned.reshape(frames // 2, rows // 2, columns // 2, width)


def solution(mesh):
    in_specs = (
        P(("groups", "tm"), "height", None, None),
        P(),
        P(None, None, "height", None),
        P(),
        P(),
        P(),
        P(),
    )
    out_specs = P(("groups", "tm"), "height", None, None)

    return jax.shard_map(body, mesh=mesh, in_specs=in_specs, out_specs=out_specs, check_vma=False)
```

```python
import jax
import jax.numpy as jnp
from jax import lax
from jax.experimental import pallas as pl
from jax.experimental.pallas import tpu as pltpu
from jax.sharding import PartitionSpec as P


HEAD_DIM = 64
CORES = 2

epsilon = 1e-06
inv_root = 0.7071067811865476

F32 = jnp.float32
BF16 = jnp.bfloat16


def dot(a, b):
    return jnp.dot(a, b, preferred_element_type=F32)


def vmem(count):
    return [pl.BlockSpec(memory_space=pltpu.VMEM) for _ in range(count)]


def params(mib=20):
    return pltpu.CompilerParams(vmem_limit_bytes=mib * 2**20)


def cost(flops, nbytes):
    return pl.CostEstimate(flops=flops, bytes_accessed=nbytes, transcendentals=0)


def hold_kernel(video_ref, gain_ref, video_held_ref, gain_held_ref, sems):
    moves = [(video_ref, video_held_ref), (gain_ref, gain_held_ref)]
    started = [pltpu.make_async_copy(src, dst, sems.at[i]) for i, (src, dst) in enumerate(moves)]
    for copy in started:
        copy.start()
    for copy in started:
        copy.wait()


def edges_kernel(earlier_ref, video_ref, first_ref, last_ref):
    frames, rows = video_ref.shape[:2]
    for i, ref in enumerate((earlier_ref, video_ref)):
        for frame in range(frames):
            first_ref[i * frames + frame] = ref[frame, 0]
            last_ref[i * frames + frame] = ref[frame, rows - 1]


def far(x):
    return pltpu.with_memory_space_constraint(x, pltpu.HBM)


def prepare_kernel(earlier_ref, video_ref, above_ref, below_ref, gain_ref, windows_ref, ordered_ref):
    frames, rows, columns, _ = video_ref.shape
    half = columns // 2
    place = lax.broadcasted_iota(jnp.int32, (3 * columns, columns), 0)
    source = lax.broadcasted_iota(jnp.int32, (3 * columns, columns), 1)
    tap, within = place // columns, place % columns
    wanted = 2 * (within % half) + within // half + tap - 1
    pick = (source == wanted).astype(F32).astype(BF16)
    gain = gain_ref[...]
    for frame in range(2 * frames):
        for row in range(rows + 2):
            if row == 0:
                block = above_ref[frame]
            elif row == rows + 1:
                block = below_ref[frame]
            elif frame < frames:
                block = earlier_ref[frame, row - 1]
            else:
                block = video_ref[frame - frames, row - 1]
                ordered_ref[frame - frames, row - 1] = dot(pick[columns : 2 * columns], block).astype(BF16)
            values = block.astype(F32)
            square = jnp.mean(values * values, axis=-1, keepdims=True)
            normed = values * lax.rsqrt(square + epsilon) * gain
            acted = (normed * jax.nn.sigmoid(normed)).astype(BF16)
            moved = dot(pick, acted).astype(BF16)
            for t in range(3):
                windows_ref[t, frame, row] = moved[t * columns : (t + 1) * columns]


def haar_rows(values, rows, half):
    out = []
    for pair in range(rows // 2):
        blocks = [
            values[f][((2 * pair + r) * 2 + c) * half : ((2 * pair + r) * 2 + c + 1) * half]
            for f in range(2)
            for r in range(2)
            for c in range(2)
        ]
        for step in (4, 2, 1):
            split = list(blocks)
            for i in range(8):
                if not i & step:
                    split[i] = (blocks[i] + blocks[i + step]) * inv_root
                    split[i + step] = (blocks[i] - blocks[i + step]) * inv_root
            blocks = split
        out.append(jnp.concatenate([b.astype(BF16) for b in blocks], axis=1))
    return jnp.concatenate(out, axis=0)


def latent_kernel(
    core_ref, own_ref, other_ref, windows_ref, video_ref, temporal_far_ref, haar_far_ref, latent_ref, temporal_ref, haar_ref, sems
):
    frames, rows, columns, channels = video_ref.shape
    chips = own_ref.shape[0]
    temporal_copy = pltpu.make_async_copy(temporal_far_ref, temporal_ref, sems.at[0])
    haar_copy = pltpu.make_async_copy(haar_far_ref, haar_ref, sems.at[1])
    temporal_copy.start()
    haar_copy.start()
    first = core_ref[0] == 0
    taps = []
    for tap in range(9):
        parts = []
        for chip in range(chips):
            own, other = own_ref[chip, tap], other_ref[chip, tap]
            parts += [jnp.where(first, own, other), jnp.where(first, other, own)]
        taps.append(jnp.concatenate(parts, axis=0))
    weights = jnp.concatenate(taps, axis=0)
    spatial = []
    for frame in range(2 * frames):
        near = [
            windows_ref[tap % 3, frame, tap // 3 : tap // 3 + rows].reshape(rows * columns, channels) for tap in range(9)
        ]
        spatial.append(dot(jnp.concatenate(near, axis=1), weights).astype(BF16))
    temporal_copy.wait()
    merged = []
    for frame in range(frames):
        total = video_ref[frame].reshape(rows * columns, channels).astype(F32)
        three = jnp.concatenate(spatial[frame : frame + 3], axis=1)
        total = total + dot(three, temporal_ref[...].reshape(3 * channels, channels))
        merged.append(total.astype(BF16).astype(F32))
    bands = haar_rows(merged, rows, columns // 2)
    haar_copy.wait()
    latent_ref[...] = dot(bands, haar_ref[...]).astype(BF16)


def attention_kernel(latent_ref, query_ref, key_ref, out_ref):
    frames = latent_ref.shape[0]
    width = query_ref.shape[0]
    places = latent_ref.shape[1] // width
    rows = places * frames
    latent = jnp.concatenate([latent_ref[:, p * width : (p + 1) * width] for p in range(places)], axis=0)
    queries = dot(latent, query_ref[...]).astype(BF16)
    keys = dot(latent, key_ref[...]).astype(BF16)
    at = lax.broadcasted_iota(jnp.int32, (rows, rows), 0)
    to = lax.broadcasted_iota(jnp.int32, (rows, rows), 1)
    allowed = (at // frames == to // frames) & (to <= at)
    pair = 2 * HEAD_DIM
    lane = lax.broadcasted_iota(jnp.int32, (rows, pair), 1)
    sides = [(lane // HEAD_DIM == i).astype(F32).astype(BF16) for i in range(2)]
    starts = range(0, width, pair)
    scores = []
    for start in starts:
        q, k = queries[:, start : start + pair], keys[:, start : start + pair]
        for side in sides:
            score = lax.dot_general(q, k * side, (((1,), (1,)), ((), ())), preferred_element_type=F32)
            scores.append(jnp.where(allowed, score * HEAD_DIM ** (-0.5), -1e30))
    scores = jnp.concatenate(scores, axis=0)
    weights = jnp.exp(scores - jnp.max(scores, axis=-1, keepdims=True))
    probs = (weights / jnp.sum(weights, axis=-1, keepdims=True)).astype(BF16)
    pieces = []
    for i, start in enumerate(starts):
        v = latent[:, start : start + pair]
        mixed = None
        for j, side in enumerate(sides):
            term = dot(probs[(2 * i + j) * rows : (2 * i + j + 1) * rows], v * side)
            mixed = term if mixed is None else mixed + term
        pieces.append((v.astype(F32) + mixed.astype(BF16).astype(F32)).astype(BF16))
    encoded = jnp.concatenate(pieces, axis=1)
    for p in range(places):
        out_ref[:, p * width : (p + 1) * width] = encoded[p * frames : (p + 1) * frames]


def body(video, norm_gain, spatial_weight, temporal_weight, haar_weight, query_weight, key_weight):
    frames, rows, columns, channels = video.shape
    outward = spatial_weight.shape[3]
    width = haar_weight.shape[1]
    height = lax.axis_size("height")
    members = lax.axis_size("tm")
    chips = height // CORES
    slice_depth = spatial_weight.shape[2]

    earlier = lax.ppermute(video, "tm", [(i, i + 1) for i in range(members - 1)])

    hold = pl.pallas_call(
        hold_kernel,
        out_shape=(
            jax.ShapeDtypeStruct(video.shape, BF16),
            jax.ShapeDtypeStruct((1, channels), F32),
        ),
        in_specs=[pl.BlockSpec(memory_space=pl.ANY)] * 2,
        out_specs=tuple(vmem(2)),
        scratch_shapes=[pltpu.SemaphoreType.DMA((2,))],
        cost_estimate=cost(10**6, 10**6),
        compiler_params=params(),
        name="hold",
    )
    held, gain = hold(far(video), far(norm_gain.reshape(1, channels)))

    slices = spatial_weight.reshape(9, slice_depth, outward)
    same_core = [[c + CORES * i for i in range(chips)] for c in range(CORES)]
    copies = jnp.broadcast_to(slices, (chips, *slices.shape))
    own = lax.all_to_all(
        copies, "height", split_axis=0, concat_axis=0, axis_index_groups=same_core, tiled=True
    )

    rims = jax.ShapeDtypeStruct((2 * frames, columns, channels), BF16)
    trim = pl.pallas_call(
        edges_kernel,
        out_shape=(rims, rims),
        in_specs=vmem(2),
        out_specs=tuple(vmem(2)),
        cost_estimate=cost(10**6, 10**6),
        compiler_params=params(),
        name="edges",
    )
    first, last = trim(earlier, held)
    above = lax.ppermute(last, "height", [(i, i + 1) for i in range(height - 1)])
    below = lax.ppermute(first, "height", [(i + 1, i) for i in range(height - 1)])
    windows, ordered = pl.pallas_call(
        prepare_kernel,
        out_shape=(
            jax.ShapeDtypeStruct((3, 2 * frames, rows + 2, columns, channels), BF16),
            jax.ShapeDtypeStruct(video.shape, BF16),
        ),
        in_specs=vmem(5),
        out_specs=tuple(vmem(2)),
        cost_estimate=cost(10**9, 4 * 10**6),
        compiler_params=params(),
        name="prepare",
    )(earlier, held, above, below, gain)

    other = lax.ppermute(own, "height", [(i, i ^ 1) for i in range(height)])
    core = (lax.axis_index("height") % CORES).astype(jnp.int32).reshape(1)
    places = (rows // 2) * (columns // 2)
    latent = pl.pallas_call(
        latent_kernel,
        out_shape=jax.ShapeDtypeStruct((places, width), BF16),
        in_specs=[pl.BlockSpec(memory_space=pltpu.SMEM)] + vmem(4) + [pl.BlockSpec(memory_space=pl.ANY)] * 2,
        out_specs=vmem(1)[0],
        scratch_shapes=[
            pltpu.VMEM(temporal_weight.shape, BF16),
            pltpu.VMEM(haar_weight.shape, BF16),
            pltpu.SemaphoreType.DMA((2,)),
        ],
        cost_estimate=cost(4 * 10**9, 8 * 10**6),
        compiler_params=params(),
        name="latent",
    )(core, own, other, windows, ordered, far(temporal_weight), far(haar_weight))

    per_member = places // members
    lanes = 128
    blocks = width // lanes
    message = (per_member * blocks, lanes)
    sent = latent.reshape(per_member, members, blocks, lanes).transpose(1, 0, 2, 3).reshape(members, *message)
    gathered = lax.all_to_all(sent, "tm", split_axis=0, concat_axis=0, tiled=True)
    encoded = pl.pallas_call(
        attention_kernel,
        out_shape=jax.ShapeDtypeStruct((members, per_member * width), BF16),
        in_specs=vmem(3),
        out_specs=vmem(1)[0],
        cost_estimate=cost(10**9, 4 * 10**6),
        compiler_params=params(),
        name="attention",
    )(gathered.reshape(members, per_member * width), query_weight, key_weight)
    returned = lax.all_to_all(
        encoded.reshape(members, *message), "tm", split_axis=0, concat_axis=0, tiled=True
    )
    returned = returned.reshape(members, per_member, blocks, lanes).transpose(1, 0, 2, 3)
    return returned.reshape(frames // 2, rows // 2, columns // 2, width)


def solution(mesh):
    in_specs = (
        P(("groups", "tm"), "height", None, None),
        P(),
        P(None, None, "height", None),
        P(),
        P(),
        P(),
        P(),
    )
    out_specs = P(("groups", "tm"), "height", None, None)

    return jax.shard_map(body, mesh=mesh, in_specs=in_specs, out_specs=out_specs, check_vma=False)
```
